128 devices in a mesh: row: 8 (over x, y_lo), col: 16 (over y_hi, z, core).
Axes of the slice: x: 4, y: 4 (y_hi: 2, y_lo: 2; y = y_hi * 2 + y_lo), z: 4, core: 2. Of those that a mesh axis runs over, the one named last changes fastest.
Arguments:
- tokens: bfloat16 [1024, 5120], P('row'), may hold values from -6 to 6
- expert_ids: int32 [1024], replicated, may hold values from 0 to 15
- modality: int32 [1024], replicated, may hold values from 0 to 1
- tile_counts: int32 [2, 16], replicated, may hold values from 1 to 4, as said below
- router: bfloat16 [5120, 16], P(None, 'col'), may hold values from -0.15625 to 0.15625
- w_gate: bfloat16 [16, 5120, 4096], P('col', None, 'row'), may hold values from -0.078125 to 0.078125
- w_up: bfloat16 [16, 5120, 4096], P('col', None, 'row'), may hold values from -0.078125 to 0.078125
- w_down: bfloat16 [16, 4096, 5120], P('col', 'row'), may hold values from -0.09375 to 0.09375
- shared_gate: bfloat16 [5120, 8192], P('row', 'col'), may hold values from -0.078125 to 0.078125
- shared_up: bfloat16 [5120, 8192], P('row', 'col'), may hold values from -0.078125 to 0.078125
- shared_down: bfloat16 [8192, 5120], P('col', 'row'), may hold values from -0.0625 to 0.0625
Outputs:
- mixed: bfloat16 [1024, 5120], P('col', 'row')
The draws below stay inside these ranges and needn't reach their ends.
Inputs may be any that keep to these rules, and one draw needn't show every extreme that they name: `tile_counts`: in every draw some expert's text segment has 4 tiles and at least 32 text tokens, and some expert's image segment has 4 tiles and at least 32 image tokens.
All inputs are finite; a program needn't handle non-finite values.
Results may differ from the reference program's by a relative error of at most 0.0052.
Values may be sent and summed in bfloat16 or wider, within the bound.
A program may use at most 128 MiB of HBM per device.

```python
import jax
import jax.numpy as jnp
from jax import lax

D = 5120
FFW = 4096
FS = 8192
TILE = 8
MAXT = 4
TOKENS = 1024
E = 16


def routing(key):
    base = jax.random.fold_in(key, 7)
    keys = jax.random.split(base, 6)
    weights = (2 ** jax.random.randint(keys[0], (E,), 0, 4)).astype(jnp.int32)
    bounds = jnp.cumsum(weights).astype(jnp.int32)
    picks = jax.random.randint(keys[1], (TOKENS,), 0, bounds[-1])
    chosen = jnp.sum((picks[:, None] >= bounds[None, :]).astype(jnp.int32), axis=1).astype(jnp.int32)
    flags = (jax.random.randint(keys[2], (TOKENS,), 0, 5) < 2).astype(jnp.int32)
    counts = jax.random.randint(keys[3], (2, E), 1, MAXT + 1).astype(jnp.int32)
    hottest = jax.random.randint(keys[4], (2,), 0, E).astype(jnp.int32)
    order = jax.random.permutation(keys[5], TOKENS)
    places = jnp.zeros((TOKENS,), jnp.int32).at[order].set(jnp.arange(TOKENS, dtype=jnp.int32))
    capacity = MAXT * TILE
    forced_text = places < capacity
    forced_image = (places >= capacity) & (places < 2 * capacity)
    chosen = jnp.where(forced_text, hottest[0], jnp.where(forced_image, hottest[1], chosen))
    flags = jnp.where(forced_text, 0, jnp.where(forced_image, 1, flags))
    counts = counts.at[0, hottest[0]].set(MAXT).at[1, hottest[1]].set(MAXT)
    return (chosen.astype(jnp.int32), flags.astype(jnp.int32), counts.astype(jnp.int32))


def draw_expert_ids(key, part):
    return routing(key)[0]


def draw_modality(key, part):
    return routing(key)[1]


def draw_tile_counts(key, part):
    return routing(key)[2]


def block_scale(own_key, dims, shards, low, high):
    factor_of = 1.0
    for axis_at, blocks in shards:
        heights = jax.random.uniform(jax.random.fold_in(jax.random.fold_in(own_key, 6), axis_at), (blocks,), jnp.float32, low / len(shards), high / len(shards))
        factor_of = factor_of * jnp.repeat(jnp.exp(heights), dims[axis_at] // blocks).reshape((-1,) + (1,) * (len(dims) - 1 - axis_at))
    return factor_of


def centred(stream_key, dims, deviation, most, cuts=(), kind=jnp.bfloat16):
    array = jax.random.normal(stream_key, dims, jnp.float32) * deviation
    if len(cuts) > 0:
        array = block_scale(stream_key, dims, cuts, -0.22, 0.18) * array
    return jnp.clip(array, min=-most, max=most).astype(kind)


def setup_inputs(seed: int = 0) -> dict:
    key_list = jax.random.split(jax.random.key(seed), 12)
    return {
        "tokens": centred(key_list[0], (TOKENS, D), 1.0, 6.0, ((0, 8),)),
        "expert_ids": draw_expert_ids(jax.random.fold_in(key_list[11], 71), 0),
        "modality": draw_modality(jax.random.fold_in(key_list[11], 71), 0),
        "tile_counts": draw_tile_counts(jax.random.fold_in(key_list[11], 71), 0),
        "router": centred(key_list[4], (D, E), (D // 4) ** -0.5, 0.15625, ((1, 16),)),
        "w_gate": centred(key_list[5], (E, D, FFW), D ** -0.5, 0.078125, ((0, 16), (2, 8))),
        "w_up": centred(key_list[6], (E, D, FFW), D ** -0.5, 0.078125, ((0, 16), (2, 8))),
        "w_down": centred(key_list[7], (E, FFW, D), FFW ** -0.5, 0.09375, ((0, 16), (1, 8))),
        "shared_gate": centred(key_list[8], (D, FS), D ** -0.5, 0.078125, ((0, 8), (1, 16))),
        "shared_up": centred(key_list[9], (D, FS), D ** -0.5, 0.078125, ((0, 8), (1, 16))),
        "shared_down": centred(key_list[10], (FS, D), FS ** -0.5, 0.0625, ((0, 16), (1, 8))),
    }


def slot_places(expert_ids, modality, tile_counts, expert):
    capacity = MAXT * TILE
    places = jnp.full(expert_ids.shape, -1, jnp.int32)
    for kind in range(2):
        member = ((expert_ids == expert) & (modality == kind)).astype(jnp.int32)
        rank = (jnp.cumsum(member, dtype=jnp.int32) - 1).astype(jnp.int32)
        limit = (tile_counts[kind, expert] * TILE).astype(jnp.int32)
        keep = (member == 1) & (rank < limit)
        places = jnp.where(keep, (kind * capacity + rank).astype(jnp.int32), places)
    return places


def slot_table(places):
    slots = lax.broadcasted_iota(jnp.int32, (2 * MAXT * TILE, places.shape[0]), 0)
    return (slots == places[None, :]).astype(jnp.bfloat16)


def place_rows(places, values):
    index = jnp.maximum(places, 0).astype(jnp.int32)
    rows = jnp.take(values, index, axis=0)
    return jnp.where((places >= 0)[:, None], rows, jnp.zeros_like(rows))


def reference(tokens, expert_ids, modality, tile_counts, router, w_gate, w_up, w_down, shared_gate, shared_up, shared_down):
    def one_expert(expert, routed):
        places = slot_places(expert_ids, modality, tile_counts, expert)
        table = slot_table(places)
        taken = jnp.dot(table, tokens, preferred_element_type=jnp.float32).astype(jnp.bfloat16)
        column = lax.dynamic_slice_in_dim(router, expert, 1, 1)
        score = jax.nn.sigmoid(jnp.dot(taken, column, preferred_element_type=jnp.float32))
        scaled = (taken.astype(jnp.float32) * score).astype(jnp.bfloat16)
        gate = jnp.dot(scaled, w_gate[expert], preferred_element_type=jnp.float32)
        upper = jnp.dot(scaled, w_up[expert], preferred_element_type=jnp.float32)
        hidden = (jax.nn.silu(gate) * upper).astype(jnp.bfloat16)
        result = jnp.dot(hidden, w_down[expert], preferred_element_type=jnp.float32)
        return routed + place_rows(places, result)

    routed = lax.fori_loop(0, E, one_expert, jnp.zeros((TOKENS, D), jnp.float32))
    shared_gate_sum = jnp.dot(tokens, shared_gate, preferred_element_type=jnp.float32)
    shared_up_sum = jnp.dot(tokens, shared_up, preferred_element_type=jnp.float32)
    shared_hidden = (jax.nn.silu(shared_gate_sum) * shared_up_sum).astype(jnp.bfloat16)
    shared = jnp.dot(shared_hidden, shared_down, preferred_element_type=jnp.float32)
    return (routed + shared).astype(jnp.bfloat16)
```

```python
import jax
import jax.numpy as jnp
from jax import lax
from jax.experimental import pallas as pl
from jax.experimental.pallas import tpu as pltpu
from jax.sharding import Mesh
from jax.sharding import PartitionSpec as P

TILE = 8
MAXT = 4
ROW = ("x", "yl")
COL = ("yh", "z", "core")
ROWS = 8
MESH = pl.DeviceIdType.MESH
BF16 = jnp.bfloat16
F32 = jnp.float32


def dot(a, b):
    return jnp.dot(a, b, preferred_element_type=F32)


def silu(v):
    return v / (1.0 + jnp.exp(-v))


def kernel(
    ids, mod, counts, tokens, router, w_gate, w_up, w_down, s_gate, s_up, s_down,
    out,
    wg, wu, wd, sg, su, sd, xs, table, place, ysend, yrecv, xsend, xrecv, taken,
    hid_e, esend, erecv, eysend, eyrecv, hilo, hid, acc, sib, zsend, zrecv, hsend, hrecv,
    load_sem, a_send, a_recv, s_send, s_recv, y_send, y_recv, x_send, x_recv, b_send, b_recv,
    e_send, e_recv, ey_send, ey_recv, d_send, d_recv, k_send, k_recv, z_send, z_recv, h_send, h_recv,
):
    x, yl, yh = lax.axis_index("x"), lax.axis_index("yl"), lax.axis_index("yh")
    z, core = lax.axis_index("z"), lax.axis_index("core")
    block, width = xs.shape[1], xs.shape[2]
    half = block // 2
    slots = table.shape[0]
    hidden = sg.shape[1]
    row = x * 2 + yl
    expert = yh * 8 + z * 2 + core

    def ahead(dx):
        return lax.rem(x + dx, 4)

    def owner(slot):
        dx, dy = slot // 2, slot % 2
        return lax.rem(x + 4 - dx, 4) * 2 + (yl + dy) % 2

    def to_row(dx, dy):
        return {"x": ahead(dx), "yl": lax.rem(yl + dy, 2)}

    sibling = {"core": 1 - core}
    other_y = {"yl": 1 - yl}

    def remote(src, dst, send, recv, device):
        return pltpu.make_async_remote_copy(
            src_ref=src, dst_ref=dst, send_sem=send, recv_sem=recv, device_id=device, device_id_type=MESH
        )

    loads = [
        pltpu.make_async_copy(tokens.at[:, pl.ds(pl.multiple_of(row * width, 128), width)], xs.at[0], load_sem.at[0]),
        pltpu.make_async_copy(s_gate, sg, load_sem.at[1]),
        pltpu.make_async_copy(s_up, su, load_sem.at[2]),
        pltpu.make_async_copy(w_gate.at[0], wg, load_sem.at[3]),
        pltpu.make_async_copy(w_up.at[0], wu, load_sem.at[4]),
        pltpu.make_async_copy(w_down.at[0], wd, load_sem.at[5]),
        pltpu.make_async_copy(s_down, sd, load_sem.at[6]),
    ]
    for load in loads:
        load.start()

    barrier = pltpu.get_barrier_semaphore()
    peers = [to_row(s // 2, s % 2) for s in range(1, ROWS)]
    peers += [{"z": lax.rem(z + dz, 4)} for dz in (1, 2, 3)] + [{"yh": 1 - yh}, sibling]
    for peer in peers:
        pl.semaphore_signal(barrier, inc=1, device_id=peer, device_id_type=MESH)

    count = ids.shape[1]
    lane = lax.broadcasted_iota(jnp.int32, (2, count), 1)
    kind = lax.broadcasted_iota(jnp.int32, (2, count), 0)
    member = (ids[...] == expert) & (mod[...] == kind)
    rank = member.astype(jnp.int32)
    step = 1
    while step < count:
        rank = rank + jnp.where(lane >= step, pltpu.roll(rank, step, 1), 0)
        step *= 2
    rank = rank - 1
    limit = jnp.where(kind == 0, counts[0, expert], counts[1, expert]) * TILE
    keep = member & (rank < limit)
    spot = jnp.where(keep, kind * (MAXT * TILE) + rank, -1)
    places = jnp.maximum(spot[0:1, :], spot[1:2, :])
    at = lax.broadcasted_iota(jnp.int32, (slots, count), 0)
    ones = (at == places).astype(F32)
    table[...] = ones.astype(BF16)
    double = jnp.concatenate([ones, ones], axis=0)
    place[...] = double.T.astype(BF16)

    pl.semaphore_wait(barrier, len(peers))

    mine = pl.ds(pl.multiple_of(core * half, half), half)
    his = pl.ds(pl.multiple_of((1 - core) * half, half), half)

    def a_copy(s):
        dx, dy = s // 2, s % 2
        target = ahead(dx) * 2 + lax.rem(yl + dy, 2)
        return remote(
            tokens.at[mine, pl.ds(pl.multiple_of(target * width, 128), width)],
            xs.at[s, mine], a_send.at[s], a_recv.at[s], to_row(dx, dy),
        )

    def s_copy(s):
        return remote(xs.at[s, mine], xs.at[s, mine], s_send.at[s], s_recv.at[s], sibling)

    def s_arrival(s):
        return remote(xs.at[s, his], xs.at[s, his], s_send.at[s], s_recv.at[s], sibling)

    order = (1, 3, 7, 5, 4, 2, 6)
    for s in order:
        a_copy(s).start()
    loads[0].wait()
    loads[1].wait()
    loads[2].wait()

    def y_copy(dx):
        return remote(ysend.at[dx], yrecv.at[dx], y_send.at[dx], y_recv.at[dx], other_y)

    def x_copy(dx):
        return remote(xsend.at[dx - 1], xrecv.at[dx - 1], x_send.at[dx - 1], x_recv.at[dx - 1], {"x": ahead(4 - dx)})

    for s in order:
        a_copy(s).wait_recv()
        s_copy(s).start()
        if s % 2 == 1:
            s_arrival(s).wait_recv()
            ysend[s // 2, :, :hidden] = dot(xs[s], sg[...]).astype(BF16)
            ysend[s // 2, :, hidden:] = dot(xs[s], su[...]).astype(BF16)
            y_copy(s // 2).start()
    for s in (4, 2, 6):
        s_arrival(s).wait_recv()

    def part_of(s):
        columns = pl.ds(pl.multiple_of(owner(s) * block, 128), block)
        return dot(table[:, columns], xs[s])

    rows = part_of(0)
    for s in range(1, ROWS):
        rows = rows + part_of(s)
    taken[0] = rows.astype(BF16)

    def b_copy(source, dx, dy):
        s = dx * 2 + dy if source == 0 else dx * 2 + 1
        return remote(taken.at[source], taken.at[s], b_send.at[s], b_recv.at[s], to_row(dx, dy))

    b_out = [b_copy(0, 0, 1), b_copy(0, 2, 0), b_copy(0, 1, 0), b_copy(0, 3, 0)]
    for copy in b_out:
        copy.start()

    def pair_sum(dx):
        y_copy(dx).wait_recv()
        s = dx * 2
        gate = dot(xs[s], sg[...]) + yrecv[dx, :, :hidden].astype(F32)
        upper = dot(xs[s], su[...]) + yrecv[dx, :, hidden:].astype(F32)
        return gate, upper

    def pair_send(dx):
        gate, upper = pair_sum(dx)
        xsend[dx - 1, :, :hidden] = gate.astype(BF16)
        xsend[dx - 1, :, hidden:] = upper.astype(BF16)
        x_copy(dx).start()

    def b_arrival(s):
        return remote(taken.at[s], taken.at[s], b_send.at[s], b_recv.at[s], other_y)

    b_arrival(1).wait_recv()
    relayed = [b_copy(1, dx, 0) for dx in (2, 1, 3)]
    for copy in relayed:
        copy.start()
    b_out += relayed
    pair_send(2)
    pair_send(1)

    for s in (2, 3, 4, 5, 6, 7):
        b_arrival(s).wait_recv()
    loads[3].wait()
    loads[4].wait()

    def score_part(s, total):
        line = router[:, pl.ds(pl.multiple_of(owner(s) * width, 128), width)].astype(F32)
        return total + jnp.sum(taken[s].astype(F32) * line, axis=1, keepdims=True)

    logit = lax.fori_loop(0, ROWS, score_part, jnp.zeros((slots, 1), F32))
    score = 1.0 / (1.0 + jnp.exp(-logit))

    def expert_part(s, sums):
        gate, upper = sums
        scaled = (taken[s].astype(F32) * score).astype(BF16)
        features = pl.ds(pl.multiple_of(owner(s) * width, 128), width)
        return gate + dot(scaled, wg[features, :]), upper + dot(scaled, wu[features, :])

    zero = jnp.zeros((slots, wg.shape[1]), F32)
    gate, upper = lax.fori_loop(0, ROWS, expert_part, (zero, zero))
    hid_e[...] = (silu(gate) * upper).astype(BF16)
    pair_send(3)
    loads[5].wait()

    def result_part(dx, dy):
        target = ahead(dx) * 2 + lax.rem(yl + dy, 2)
        return dot(hid_e[...], wd[:, pl.ds(pl.multiple_of(target * width, 128), width)])

    def e_copy(dx):
        return remote(esend.at[dx - 1], erecv.at[dx - 1], e_send.at[dx - 1], e_recv.at[dx - 1], {"x": ahead(dx)})

    for dx in (2, 1, 3):
        esend[dx - 1, 0] = result_part(dx, 0).astype(BF16)
        esend[dx - 1, 1] = result_part(dx, 1).astype(BF16)
        e_copy(dx).start()

    gate, upper = pair_sum(0)
    for dx in (2, 1, 3):
        x_copy(dx).wait_recv()
        gate = gate + xrecv[dx - 1, :, :hidden].astype(F32)
        upper = upper + xrecv[dx - 1, :, hidden:].astype(F32)
    hid[0] = (silu(gate) * upper).astype(BF16)

    def d_copy(source, dx, dy):
        s = dx * 2 + dy if source == 0 else dx * 2 + 1
        return remote(hid.at[source], hid.at[s], d_send.at[s], d_recv.at[s], to_row(dx, dy))

    def d_arrival(s):
        return remote(hid.at[s], hid.at[s], d_send.at[s], d_recv.at[s], other_y)

    d_out = [d_copy(0, 0, 1), d_copy(0, 2, 0), d_copy(0, 1, 0), d_copy(0, 3, 0)]
    for copy in d_out:
        copy.start()

    total = result_part(0, 0)
    passed = result_part(0, 1)
    for dx in (2, 1, 3):
        e_copy(dx).wait_recv()
        total = total + erecv[dx - 1, 0].astype(F32)
        passed = passed + erecv[dx - 1, 1].astype(F32)
    eysend[...] = passed.astype(BF16)
    ey_copy = remote(eysend, eyrecv, ey_send, ey_recv, other_y)
    ey_copy.start()
    d_arrival(1).wait_recv()
    relayed = [d_copy(1, dx, 0) for dx in (2, 1, 3)]
    for copy in relayed:
        copy.start()
    d_out += relayed
    ey_copy.wait_recv()
    total = total + eyrecv[...].astype(F32)
    high = total.astype(BF16)
    hilo[:slots] = high
    hilo[slots:] = (total - high.astype(F32)).astype(BF16)
    loads[6].wait()

    def k_copy(s):
        j = owner(s)
        return remote(acc.at[j, his], sib.at[j], k_send.at[s], k_recv.at[s], sibling)

    arrivals = (0, 1, 2, 6, 4, 3, 7, 5)
    for s in arrivals:
        if s > 1:
            d_arrival(s).wait_recv()
        j = owner(s)
        tokens_of = pl.ds(pl.multiple_of(j * block, 128), block)
        acc[j] = dot(hid[s], sd[...]) + dot(place[tokens_of, :], hilo[...])
        k_copy(s).start()
    for s in arrivals:
        k_copy(s).wait_recv()

    def chip_sum(dz, dyh):
        j = lax.rem(yh + dyh, 2) * 4 + lax.rem(z + dz, 4)
        return acc[j, mine] + sib[j]

    def z_copy(dz):
        return remote(
            zsend.at[dz - 1], zrecv.at[dz - 1], z_send.at[dz - 1], z_recv.at[dz - 1], {"z": lax.rem(z + dz, 4)}
        )

    for dz in (2, 1, 3):
        zsend[dz - 1, 0] = chip_sum(dz, 0).astype(BF16)
        zsend[dz - 1, 1] = chip_sum(dz, 1).astype(BF16)
        z_copy(dz).start()
    total = chip_sum(0, 0)
    passed = chip_sum(0, 1)
    for dz in (2, 1, 3):
        z_copy(dz).wait_recv()
        total = total + zrecv[dz - 1, 0].astype(F32)
        passed = passed + zrecv[dz - 1, 1].astype(F32)
    hsend[...] = passed.astype(BF16)
    h_copy = remote(hsend, hrecv, h_send, h_recv, {"yh": 1 - yh})
    h_copy.start()
    h_copy.wait_recv()
    out[...] = (total + hrecv[...].astype(F32)).astype(BF16)

    for s in order:
        a_copy(s).wait_send()
        s_copy(s).wait_send()
    for dx in range(4):
        y_copy(dx).wait_send()
    for dx in (1, 2, 3):
        x_copy(dx).wait_send()
        e_copy(dx).wait_send()
        z_copy(dx).wait_send()
    for copy in b_out + d_out:
        copy.wait_send()
    for s in arrivals:
        k_copy(s).wait_send()
    ey_copy.wait_send()
    h_copy.wait_send()


def per_device(tokens, expert_ids, modality, tile_counts, router, w_gate, w_up, w_down, shared_gate, shared_up, shared_down):
    block, depth = tokens.shape
    width = shared_down.shape[1]
    hidden = shared_gate.shape[1]
    inner = w_gate.shape[2]
    slots = 2 * MAXT * TILE
    half = block // 2
    count = expert_ids.shape[0]
    vmem = pl.BlockSpec(memory_space=pltpu.VMEM)
    hbm = pl.BlockSpec(memory_space=pl.ANY)
    dma = pltpu.SemaphoreType.DMA
    return pl.pallas_call(
        kernel,
        name="layer",
        out_shape=jax.ShapeDtypeStruct((half, width), BF16),
        in_specs=[vmem, vmem, pl.BlockSpec(memory_space=pltpu.SMEM), hbm, vmem] + [hbm] * 6,
        out_specs=vmem,
        scratch_shapes=[
            pltpu.VMEM((depth, inner), BF16),
            pltpu.VMEM((depth, inner), BF16),
            pltpu.VMEM((inner, depth), BF16),
            pltpu.VMEM((width, hidden), BF16),
            pltpu.VMEM((width, hidden), BF16),
            pltpu.VMEM((hidden, width), BF16),
            pltpu.VMEM((ROWS, block, width), BF16),
            pltpu.VMEM((slots, count), BF16),
            pltpu.VMEM((count, 2 * slots), BF16),
            pltpu.VMEM((4, block, 2 * hidden), BF16),
            pltpu.VMEM((4, block, 2 * hidden), BF16),
            pltpu.VMEM((3, block, 2 * hidden), BF16),
            pltpu.VMEM((3, block, 2 * hidden), BF16),
            pltpu.VMEM((ROWS, slots, width), BF16),
            pltpu.VMEM((slots, inner), BF16),
            pltpu.VMEM((3, 2, slots, width), BF16),
            pltpu.VMEM((3, 2, slots, width), BF16),
            pltpu.VMEM((slots, width), BF16),
            pltpu.VMEM((slots, width), BF16),
            pltpu.VMEM((2 * slots, width), BF16),
            pltpu.VMEM((ROWS, block, hidden), BF16),
            pltpu.VMEM((ROWS, block, width), F32),
            pltpu.VMEM((ROWS, half, width), F32),
            pltpu.VMEM((3, 2, half, width), BF16),
            pltpu.VMEM((3, 2, half, width), BF16),
            pltpu.VMEM((half, width), BF16),
            pltpu.VMEM((half, width), BF16),
            dma((7,)),
            dma((ROWS,)), dma((ROWS,)), dma((ROWS,)), dma((ROWS,)),
            dma((4,)), dma((4,)), dma((3,)), dma((3,)),
            dma((ROWS,)), dma((ROWS,)),
            dma((3,)), dma((3,)), dma, dma,
            dma((ROWS,)), dma((ROWS,)), dma((ROWS,)), dma((ROWS,)),
            dma((3,)), dma((3,)), dma, dma,
        ],
        compiler_params=pltpu.CompilerParams(
            collective_id=0, has_side_effects=True, vmem_limit_bytes=60 * 1024 * 1024
        ),
    )(
        expert_ids.reshape(1, count), modality.reshape(1, count), tile_counts, tokens, router.reshape(1, depth),
        w_gate, w_up, w_down, shared_gate, shared_up, shared_down,
    )


def solution(mesh):
    split = Mesh(mesh.devices.reshape(4, 2, 2, 4, 2), ("x", "yl", "yh", "z", "core"))
    placed = (
        P(ROW, None),
        P(),
        P(),
        P(),
        P(None, COL),
        P(COL, None, ROW),
        P(COL, None, ROW),
        P(COL, ROW, None),
        P(ROW, COL),
        P(ROW, COL),
        P(COL, ROW),
    )
    return jax.shard_map(
        per_device, mesh=split, in_specs=placed, out_specs=P(COL, ROW), check_vma=False
    )
```

```python
import jax
import jax.numpy as jnp
from jax import lax
from jax.experimental import pallas as pl
from jax.experimental.pallas import tpu as pltpu
from jax.sharding import Mesh
from jax.sharding import PartitionSpec as P

TILE = 8
MAXT = 4
ROW = ("x", "yl")
COL = ("yh", "z", "core")
ROWS = 8
MESH = pl.DeviceIdType.MESH
BF16 = jnp.bfloat16
F32 = jnp.float32


def dot(a, b):
    return jnp.dot(a, b, preferred_element_type=F32)


def silu(v):
    return v / (1.0 + jnp.exp(-v))


def kernel(
    ids, mod, counts, tokens, router, w_gate, w_up, w_down, s_gate, s_up, s_down,
    out,
    wg, wu, wd, sg, su, sd, xs, table, place, ysend, yrecv, xsend, xrecv, taken,
    hid_e, esend, erecv, eysend, eyrecv, hilo, hid, acc, sib, own, zsend, zrecv, hsend, hrecv,
    load_sem, a_send, a_recv, s_send, s_recv, y_send, y_recv, x_send, x_recv, b_send, b_recv,
    e_send, e_recv, ey_send, ey_recv, d_send, d_recv, k_send, k_recv, z_send, z_recv, h_send, h_recv,
):
    x, yl, yh = lax.axis_index("x"), lax.axis_index("yl"), lax.axis_index("yh")
    z, core = lax.axis_index("z"), lax.axis_index("core")
    block, width = xs.shape[1], xs.shape[2]
    half = block // 2
    slots = table.shape[0]
    hidden = sg.shape[1]
    row = x * 2 + yl
    expert = yh * 8 + z * 2 + core

    def ahead(dx):
        return lax.rem(x + dx, 4)

    def owner(slot):
        dx, dy = slot // 2, slot % 2
        return lax.rem(x + 4 - dx, 4) * 2 + (yl + dy) % 2

    def to_row(dx, dy):
        return {"x": ahead(dx), "yl": lax.rem(yl + dy, 2)}

    sibling = {"core": 1 - core}
    other_y = {"yl": 1 - yl}

    def remote(src, dst, send, recv, device):
        return pltpu.make_async_remote_copy(
            src_ref=src, dst_ref=dst, send_sem=send, recv_sem=recv, device_id=device, device_id_type=MESH
        )

    loads = [
        pltpu.make_async_copy(tokens.at[:, pl.ds(pl.multiple_of(row * width, 128), width)], xs.at[0], load_sem.at[0]),
        pltpu.make_async_copy(s_gate, sg, load_sem.at[1]),
        pltpu.make_async_copy(s_up, su, load_sem.at[2]),
        pltpu.make_async_copy(w_gate.at[0], wg, load_sem.at[3]),
        pltpu.make_async_copy(w_up.at[0], wu, load_sem.at[4]),
        pltpu.make_async_copy(w_down.at[0], wd, load_sem.at[5]),
        pltpu.make_async_copy(s_down, sd, load_sem.at[6]),
    ]
    for load in loads:
        load.start()

    barrier = pltpu.get_barrier_semaphore()
    peers = [to_row(s // 2, s % 2) for s in range(1, ROWS)]
    peers += [{"z": lax.rem(z + dz, 4)} for dz in (1, 2, 3)] + [{"yh": 1 - yh}, sibling]
    for peer in peers:
        pl.semaphore_signal(barrier, inc=1, device_id=peer, device_id_type=MESH)

    count = ids.shape[1]
    lane = lax.broadcasted_iota(jnp.int32, (2, count), 1)
    kind = lax.broadcasted_iota(jnp.int32, (2, count), 0)
    member = (ids[...] == expert) & (mod[...] == kind)
    rank = member.astype(jnp.int32)
    step = 1
    while step < count:
        rank = rank + jnp.where(lane >= step, pltpu.roll(rank, step, 1), 0)
        step *= 2
    rank = rank - 1
    limit = jnp.where(kind == 0, counts[0, expert], counts[1, expert]) * TILE
    keep = member & (rank < limit)
    spot = jnp.where(keep, kind * (MAXT * TILE) + rank, -1)
    places = jnp.maximum(spot[0:1, :], spot[1:2, :])
    at = lax.broadcasted_iota(jnp.int32, (slots, count), 0)
    ones = (at == places).astype(F32)
    table[...] = ones.astype(BF16)
    double = jnp.concatenate([ones, ones], axis=0)
    place[...] = double.T.astype(BF16)

    pl.semaphore_wait(barrier, len(peers))

    mine = pl.ds(pl.multiple_of(core * half, half), half)
    his = pl.ds(pl.multiple_of((1 - core) * half, half), half)

    def a_copy(s):
        dx, dy = s // 2, s % 2
        target = ahead(dx) * 2 + lax.rem(yl + dy, 2)
        return remote(
            tokens.at[mine, pl.ds(pl.multiple_of(target * width, 128), width)],
            xs.at[s, mine], a_send.at[s], a_recv.at[s], to_row(dx, dy),
        )

    def s_copy(s):
        return remote(xs.at[s, mine], xs.at[s, mine], s_send.at[s], s_recv.at[s], sibling)

    def s_arrival(s):
        return remote(xs.at[s, his], xs.at[s, his], s_send.at[s], s_recv.at[s], sibling)

    order = (5, 3, 7, 1, 4, 2, 6)
    for s in order:
        a_copy(s).start()
    loads[0].wait()

    def y_copy(dx):
        return remote(ysend.at[dx], yrecv.at[dx], y_send.at[dx], y_recv.at[dx], other_y)

    def x_copy(dx):
        return remote(xsend.at[dx - 1], xrecv.at[dx - 1], x_send.at[dx - 1], x_recv.at[dx - 1], {"x": ahead(4 - dx)})

    for s in order:
        a_copy(s).wait_recv()
        s_copy(s).start()

    def part_of(s):
        columns = pl.ds(pl.multiple_of(owner(s) * block, 128), block)
        return dot(table[:, columns], xs[s])

    rows = part_of(0)
    for s in order:
        s_arrival(s).wait_recv()
        rows = rows + part_of(s)
    taken[0] = rows.astype(BF16)

    def b_copy(source, dx, dy):
        s = dx * 2 + dy if source == 0 else dx * 2 + 1
        return remote(taken.at[source], taken.at[s], b_send.at[s], b_recv.at[s], to_row(dx, dy))

    def b_arrival(s):
        return remote(taken.at[s], taken.at[s], b_send.at[s], b_recv.at[s], other_y)

    b_out = [b_copy(0, 0, 1), b_copy(0, 2, 0), b_copy(0, 1, 0), b_copy(0, 3, 0)]
    for copy in b_out:
        copy.start()

    loads[1].wait()
    loads[2].wait()
    for dx in (2, 1, 3, 0):
        s = dx * 2 + 1
        ysend[dx, :, :hidden] = dot(xs[s], sg[...]).astype(BF16)
        ysend[dx, :, hidden:] = dot(xs[s], su[...]).astype(BF16)
        y_copy(dx).start()

    b_arrival(1).wait_recv()
    relayed = [b_copy(1, dx, 0) for dx in (2, 1, 3)]
    for copy in relayed:
        copy.start()
    b_out += relayed

    def pair_sum(dx):
        y_copy(dx).wait_recv()
        s = dx * 2
        gate = dot(xs[s], sg[...]) + yrecv[dx, :, :hidden].astype(F32)
        upper = dot(xs[s], su[...]) + yrecv[dx, :, hidden:].astype(F32)
        return gate, upper

    def pair_send(dx):
        gate, upper = pair_sum(dx)
        xsend[dx - 1, :, :hidden] = gate.astype(BF16)
        xsend[dx - 1, :, hidden:] = upper.astype(BF16)
        x_copy(dx).start()

    pair_send(2)
    pair_send(1)

    for s in (2, 3, 4, 5, 6, 7):
        b_arrival(s).wait_recv()
    loads[3].wait()
    loads[4].wait()

    def score_part(s, total):
        line = router[:, pl.ds(pl.multiple_of(owner(s) * width, 128), width)].astype(F32)
        return total + jnp.sum(taken[s].astype(F32) * line, axis=1, keepdims=True)

    logit = lax.fori_loop(0, ROWS, score_part, jnp.zeros((slots, 1), F32))
    score = 1.0 / (1.0 + jnp.exp(-logit))

    def expert_part(s, sums):
        gate, upper = sums
        scaled = (taken[s].astype(F32) * score).astype(BF16)
        features = pl.ds(pl.multiple_of(owner(s) * width, 128), width)
        return gate + dot(scaled, wg[features, :]), upper + dot(scaled, wu[features, :])

    zero = jnp.zeros((slots, wg.shape[1]), F32)
    gate, upper = lax.fori_loop(0, ROWS, expert_part, (zero, zero))
    hid_e[...] = (silu(gate) * upper).astype(BF16)
    pair_send(3)
    loads[5].wait()

    def result_part(dx, dy):
        target = ahead(dx) * 2 + lax.rem(yl + dy, 2)
        return dot(hid_e[...], wd[:, pl.ds(pl.multiple_of(target * width, 128), width)])

    def e_copy(dx):
        return remote(esend.at[dx - 1], erecv.at[dx - 1], e_send.at[dx - 1], e_recv.at[dx - 1], {"x": ahead(dx)})

    for dx in (2, 1, 3):
        esend[dx - 1, 0] = result_part(dx, 0).astype(BF16)
        esend[dx - 1, 1] = result_part(dx, 1).astype(BF16)
        e_copy(dx).start()

    gate, upper = pair_sum(0)
    for dx in (2, 1, 3):
        x_copy(dx).wait_recv()
        gate = gate + xrecv[dx - 1, :, :hidden].astype(F32)
        upper = upper + xrecv[dx - 1, :, hidden:].astype(F32)
    hid[0] = (silu(gate) * upper).astype(BF16)

    def d_copy(source, dx, dy):
        s = dx * 2 + dy if source == 0 else dx * 2 + 1
        return remote(hid.at[source], hid.at[s], d_send.at[s], d_recv.at[s], to_row(dx, dy))

    def d_arrival(s):
        return remote(hid.at[s], hid.at[s], d_send.at[s], d_recv.at[s], other_y)

    d_out = [d_copy(0, 0, 1), d_copy(0, 2, 0), d_copy(0, 1, 0), d_copy(0, 3, 0)]
    for copy in d_out:
        copy.start()

    total = result_part(0, 0)
    passed = result_part(0, 1)
    for dx in (2, 1, 3):
        e_copy(dx).wait_recv()
        total = total + erecv[dx - 1, 0].astype(F32)
        passed = passed + erecv[dx - 1, 1].astype(F32)
    eysend[...] = passed.astype(BF16)
    ey_copy = remote(eysend, eyrecv, ey_send, ey_recv, other_y)
    ey_copy.start()
    d_arrival(1).wait_recv()
    relayed = [d_copy(1, dx, 0) for dx in (2, 1, 3)]
    for copy in relayed:
        copy.start()
    d_out += relayed
    ey_copy.wait_recv()
    total = total + eyrecv[...].astype(F32)
    high = total.astype(BF16)
    hilo[:slots] = high
    hilo[slots:] = (total - high.astype(F32)).astype(BF16)
    loads[6].wait()

    def k_copy(s):
        return remote(acc.at[s, his], sib.at[s], k_send.at[s], k_recv.at[s], sibling)

    def place_of(s):
        j = owner(s)
        return lax.rem(lax.rem(j, 4) + 4 - z, 4), lax.rem(j // 4 + yh, 2)

    def z_copy(dz, dyh, s):
        return remote(
            zsend.at[s], zrecv.at[dz - 1, dyh], z_send.at[dz - 1, dyh], z_recv.at[dz - 1, dyh], {"z": lax.rem(z + dz, 4)}
        )

    def pass_on(s):
        k_copy(s).wait_recv()
        dz, dyh = place_of(s)
        total = acc[s, mine] + sib[s]

        @pl.when(dz == 0)
        def _():
            own[dyh] = total

        @pl.when(dz > 0)
        def _():
            zsend[s] = total.astype(BF16)
            z_copy(dz, dyh, s).start()

    arrivals = (0, 1, 4, 2, 6, 5, 3, 7)
    for i, s in enumerate(arrivals):
        if s > 1:
            d_arrival(s).wait_recv()
        tokens_of = pl.ds(pl.multiple_of(owner(s) * block, 128), block)
        acc[s] = dot(hid[s], sd[...]) + dot(place[tokens_of, :], hilo[...])
        k_copy(s).start()
        if i > 0:
            pass_on(arrivals[i - 1])
    pass_on(arrivals[-1])

    def z_sum(dyh):
        total = own[dyh]
        for dz in (1, 2, 3):
            z_copy(dz, dyh, 0).wait_recv()
            total = total + zrecv[dz - 1, dyh].astype(F32)
        return total

    hsend[...] = z_sum(1).astype(BF16)
    h_copy = remote(hsend, hrecv, h_send, h_recv, {"yh": 1 - yh})
    h_copy.start()
    total = z_sum(0)
    h_copy.wait_recv()
    out[...] = (total + hrecv[...].astype(F32)).astype(BF16)

    for s in order:
        a_copy(s).wait_send()
        s_copy(s).wait_send()
    for dx in range(4):
        y_copy(dx).wait_send()
    for dx in (1, 2, 3):
        x_copy(dx).wait_send()
        e_copy(dx).wait_send()
        z_copy(dx, 0, 0).wait_send()
        z_copy(dx, 1, 0).wait_send()
    for copy in b_out + d_out:
        copy.wait_send()
    for s in arrivals:
        k_copy(s).wait_send()
    ey_copy.wait_send()
    h_copy.wait_send()


def per_device(tokens, expert_ids, modality, tile_counts, router, w_gate, w_up, w_down, shared_gate, shared_up, shared_down):
    block, depth = tokens.shape
    width = shared_down.shape[1]
    hidden = shared_gate.shape[1]
    inner = w_gate.shape[2]
    slots = 2 * MAXT * TILE
    half = block // 2
    count = expert_ids.shape[0]
    vmem = pl.BlockSpec(memory_space=pltpu.VMEM)
    hbm = pl.BlockSpec(memory_space=pl.ANY)
    dma = pltpu.SemaphoreType.DMA
    return pl.pallas_call(
        kernel,
        name="layer",
        out_shape=jax.ShapeDtypeStruct((half, width), BF16),
        in_specs=[vmem, vmem, pl.BlockSpec(memory_space=pltpu.SMEM), hbm, vmem] + [hbm] * 6,
        out_specs=vmem,
        scratch_shapes=[
            pltpu.VMEM((depth, inner), BF16),
            pltpu.VMEM((depth, inner), BF16),
            pltpu.VMEM((inner, depth), BF16),
            pltpu.VMEM((width, hidden), BF16),
            pltpu.VMEM((width, hidden), BF16),
            pltpu.VMEM((hidden, width), BF16),
            pltpu.VMEM((ROWS, block, width), BF16),
            pltpu.VMEM((slots, count), BF16),
            pltpu.VMEM((count, 2 * slots), BF16),
            pltpu.VMEM((4, block, 2 * hidden), BF16),
            pltpu.VMEM((4, block, 2 * hidden), BF16),
            pltpu.VMEM((3, block, 2 * hidden), BF16),
            pltpu.VMEM((3, block, 2 * hidden), BF16),
            pltpu.VMEM((ROWS, slots, width), BF16),
            pltpu.VMEM((slots, inner), BF16),
            pltpu.VMEM((3, 2, slots, width), BF16),
            pltpu.VMEM((3, 2, slots, width), BF16),
            pltpu.VMEM((slots, width), BF16),
            pltpu.VMEM((slots, width), BF16),
            pltpu.VMEM((2 * slots, width), BF16),
            pltpu.VMEM((ROWS, block, hidden), BF16),
            pltpu.VMEM((ROWS, block, width), F32),
            pltpu.VMEM((ROWS, half, width), F32),
            pltpu.VMEM((2, half, width), F32),
            pltpu.VMEM((ROWS, half, width), BF16),
            pltpu.VMEM((3, 2, half, width), BF16),
            pltpu.VMEM((half, width), BF16),
            pltpu.VMEM((half, width), BF16),
            dma((7,)),
            dma((ROWS,)), dma((ROWS,)), dma((ROWS,)), dma((ROWS,)),
            dma((4,)), dma((4,)), dma((3,)), dma((3,)),
            dma((ROWS,)), dma((ROWS,)),
            dma((3,)), dma((3,)), dma, dma,
            dma((ROWS,)), dma((ROWS,)), dma((ROWS,)), dma((ROWS,)),
            dma((3, 2)), dma((3, 2)), dma, dma,
        ],
        compiler_params=pltpu.CompilerParams(
            collective_id=0, has_side_effects=True, vmem_limit_bytes=60 * 1024 * 1024
        ),
    )(
        expert_ids.reshape(1, count), modality.reshape(1, count), tile_counts, tokens, router.reshape(1, depth),
        w_gate, w_up, w_down, shared_gate, shared_up, shared_down,
    )


def solution(mesh):
    split = Mesh(mesh.devices.reshape(4, 2, 2, 4, 2), ("x", "yl", "yh", "z", "core"))
    placed = (
        P(ROW, None),
        P(),
        P(),
        P(),
        P(None, COL),
        P(COL, None, ROW),
        P(COL, None, ROW),
        P(COL, ROW, None),
        P(ROW, COL),
        P(ROW, COL),
        P(COL, ROW),
    )
    return jax.shard_map(
        per_device, mesh=split, in_specs=placed, out_specs=P(COL, ROW), check_vma=False
    )
```

```python
import jax
import jax.numpy as jnp
from jax import lax
from jax.experimental import pallas as pl
from jax.experimental.pallas import tpu as pltpu
from jax.sharding import Mesh
from jax.sharding import PartitionSpec as P

TILE = 8
MAXT = 4
ROW = ("x", "yl")
COL = ("yh", "z", "core")
ROWS = 8
MESH = pl.DeviceIdType.MESH
BF16 = jnp.bfloat16
F32 = jnp.float32


def dot(a, b):
    return jnp.dot(a, b, preferred_element_type=F32)


def silu(v):
    return v / (1.0 + jnp.exp(-v))


def kernel(
    ids, mod, counts, tokens, router, w_gate, w_up, w_down, s_gate, s_up, s_down,
    out,
    wg, wu, wd, sg, su, sd, xs, table, place, ysend, yrecv, xsend, xrecv, taken,
    hid_e, eysend, eyrecv, exsend, exrecv, hilo, mine_h, hid, own, fsend, frecv,
    load_sem, a_send, a_recv, s_send, s_recv, y_send, y_recv, x_send, x_recv, b_send, b_recv,
    ey_send, ey_recv, ex_send, ex_recv, d_send, d_recv, w_send, w_recv, k_send, k_recv, f_send, f_recv,
):
    x, yl, yh = lax.axis_index("x"), lax.axis_index("yl"), lax.axis_index("yh")
    z, core = lax.axis_index("z"), lax.axis_index("core")
    block, width = xs.shape[1], xs.shape[2]
    half = block // 2
    slots = table.shape[0]
    chunk = mine_h.shape[2]
    row = x * 2 + yl
    expert = yh * 8 + z * 2 + core

    def ahead(dx):
        return lax.rem(x + dx, 4)

    def owner(slot):
        dx, dy = slot // 2, slot % 2
        return lax.rem(x + 4 - dx, 4) * 2 + (yl + dy) % 2

    def to_row(dx, dy):
        return {"x": ahead(dx), "yl": lax.rem(yl + dy, 2)}

    sibling = {"core": 1 - core}
    other_y = {"yl": 1 - yl}

    def remote(src, dst, send, recv, device):
        return pltpu.make_async_remote_copy(
            src_ref=src, dst_ref=dst, send_sem=send, recv_sem=recv, device_id=device, device_id_type=MESH
        )

    units = pl.ds(pl.multiple_of(core * chunk, chunk), chunk)

    loads = [
        pltpu.make_async_copy(tokens.at[:, pl.ds(pl.multiple_of(row * width, 128), width)], xs.at[0], load_sem.at[0]),
        pltpu.make_async_copy(s_gate, sg, load_sem.at[1]),
        pltpu.make_async_copy(s_up, su, load_sem.at[2]),
        pltpu.make_async_copy(w_gate.at[0], wg, load_sem.at[3]),
        pltpu.make_async_copy(w_up.at[0], wu, load_sem.at[4]),
        pltpu.make_async_copy(w_down.at[0], wd, load_sem.at[5]),
        pltpu.make_async_copy(s_down.at[:chunk], sd.at[0, units], load_sem.at[6]),
        pltpu.make_async_copy(s_down.at[chunk:], sd.at[1, units], load_sem.at[7]),
    ]
    for load in loads:
        load.start()

    barrier = pltpu.get_barrier_semaphore()
    peers = [to_row(s // 2, s % 2) for s in range(1, ROWS)]
    peers += [to_row(s // 2, s % 2) | sibling for s in (1, 2, 4, 6)] + [sibling]
    peers += [{"yh": lax.rem(yh + q // 4, 2), "z": lax.rem(z + q % 4, 4)} for q in range(1, 8)]
    for peer in peers:
        pl.semaphore_signal(barrier, inc=1, device_id=peer, device_id_type=MESH)

    count = ids.shape[1]
    lane = lax.broadcasted_iota(jnp.int32, (2, count), 1)
    kind = lax.broadcasted_iota(jnp.int32, (2, count), 0)
    at = lax.broadcasted_iota(jnp.int32, (slots, count), 0)

    def ones_of(expert):
        member = (ids[...] == expert) & (mod[...] == kind)
        rank = member.astype(jnp.int32)
        step = 1
        while step < count:
            rank = rank + jnp.where(lane >= step, pltpu.roll(rank, step, 1), 0)
            step *= 2
        rank = rank - 1
        limit = jnp.where(kind == 0, counts[0, expert], counts[1, expert]) * TILE
        spot = jnp.where(member & (rank < limit), kind * (MAXT * TILE) + rank, -1)
        return (at == jnp.maximum(spot[0:1, :], spot[1:2, :])).astype(F32)

    ones = ones_of(expert)
    table[...] = ones.astype(BF16)
    place[:, : 2 * slots] = jnp.concatenate([ones, ones], axis=0).T.astype(BF16)

    pl.semaphore_wait(barrier, len(peers))

    mine = pl.ds(pl.multiple_of(core * half, half), half)
    his = pl.ds(pl.multiple_of((1 - core) * half, half), half)

    def a_copy(s):
        dx, dy = s // 2, s % 2
        target = ahead(dx) * 2 + lax.rem(yl + dy, 2)
        return remote(
            tokens.at[mine, pl.ds(pl.multiple_of(target * width, 128), width)],
            xs.at[s, mine], a_send.at[s], a_recv.at[s], to_row(dx, dy),
        )

    def s_copy(s):
        return remote(xs.at[s, mine], xs.at[s, mine], s_send.at[s], s_recv.at[s], sibling)

    def s_arrival(s):
        return remote(xs.at[s, his], xs.at[s, his], s_send.at[s], s_recv.at[s], sibling)

    order = (5, 3, 7, 1, 4, 2, 6)
    for s in order:
        a_copy(s).start()
    loads[0].wait()

    def y_copy(q, dx):
        return remote(ysend.at[q, dx], yrecv.at[q, dx], y_send.at[q, dx], y_recv.at[q, dx], other_y)

    def x_copy(q, dx):
        return remote(
            xsend.at[q, dx - 1], xrecv.at[q, dx - 1], x_send.at[q, dx - 1], x_recv.at[q, dx - 1], {"x": ahead(4 - dx)}
        )

    w_out = [
        remote(s_down.at[q * chunk : (q + 1) * chunk], sd.at[q, units], w_send.at[q], w_recv.at[q], sibling)
        for q in (0, 1)
    ]
    for copy in w_out:
        copy.start()
    ones = ones_of(yh * 8 + z * 2 + 1 - core)
    place[:, 2 * slots :] = jnp.concatenate([ones, ones], axis=0).T.astype(BF16)

    def part(q, s):
        columns = slice(q * chunk, (q + 1) * chunk)
        return dot(xs[s], sg[:, columns]), dot(xs[s], su[:, columns])

    def y_start(q, dx):
        gate, upper = part(q, dx * 2 + 1)
        ysend[q, dx, :, :chunk] = gate.astype(BF16)
        ysend[q, dx, :, chunk:] = upper.astype(BF16)
        y_copy(q, dx).start()

    loads[1].wait()
    loads[2].wait()
    for s in order[:2]:
        a_copy(s).wait_recv()
        s_copy(s).start()
    s_arrival(order[0]).wait_recv()
    y_start(0, 2)
    for s in order[2:]:
        a_copy(s).wait_recv()
        s_copy(s).start()

    def part_of(s):
        columns = pl.ds(pl.multiple_of(owner(s) * block, 128), block)
        return dot(table[:, columns], xs[s])

    rows = part_of(0)
    for i, s in enumerate(order):
        if i > 0:
            s_arrival(s).wait_recv()
        rows = rows + part_of(s)
    taken[0] = rows.astype(BF16)

    def b_copy(source, dx, dy):
        s = dx * 2 + dy if source == 0 else dx * 2 + 1
        return remote(taken.at[source], taken.at[s], b_send.at[s], b_recv.at[s], to_row(dx, dy))

    def b_arrival(s):
        return remote(taken.at[s], taken.at[s], b_send.at[s], b_recv.at[s], other_y)

    b_out = [b_copy(0, 0, 1), b_copy(0, 2, 0), b_copy(0, 1, 0), b_copy(0, 3, 0)]
    for copy in b_out:
        copy.start()

    for q, dx in ((0, 1), (0, 3), (0, 0), (1, 2), (1, 1)):
        y_start(q, dx)

    def pair_sum(q, dx):
        y_copy(q, dx).wait_recv()
        gate, upper = part(q, dx * 2)
        return gate + yrecv[q, dx, :, :chunk].astype(F32), upper + yrecv[q, dx, :, chunk:].astype(F32)

    def pair_send(q, dx):
        gate, upper = pair_sum(q, dx)
        xsend[q, dx - 1, :, :chunk] = gate.astype(BF16)
        xsend[q, dx - 1, :, chunk:] = upper.astype(BF16)
        x_copy(q, dx).start()

    b_arrival(1).wait_recv()
    relayed = [b_copy(1, dx, 0) for dx in (2, 1, 3)]
    for copy in relayed:
        copy.start()
    b_out += relayed
    for dx in (2, 1, 3):
        pair_send(0, dx)

    for s in (2, 3, 4, 5, 6, 7):
        b_arrival(s).wait_recv()
    loads[3].wait()
    loads[4].wait()

    def score_part(s, total):
        line = router[:, pl.ds(pl.multiple_of(owner(s) * width, 128), width)].astype(F32)
        return total + jnp.sum(taken[s].astype(F32) * line, axis=1, keepdims=True)

    logit = lax.fori_loop(0, ROWS, score_part, jnp.zeros((slots, 1), F32))
    score = 1.0 / (1.0 + jnp.exp(-logit))

    def expert_part(s, sums):
        gate, upper = sums
        scaled = (taken[s].astype(F32) * score).astype(BF16)
        features = pl.ds(pl.multiple_of(owner(s) * width, 128), width)
        return gate + dot(scaled, wg[features, :]), upper + dot(scaled, wu[features, :])

    zero = jnp.zeros((slots, wg.shape[1]), F32)
    gate, upper = lax.fori_loop(0, ROWS, expert_part, (zero, zero))
    hid_e[...] = (silu(gate) * upper).astype(BF16)

    def d_copy(q, s, cross):
        target = to_row(s // 2, s % 2) | ({"core": 1 - core} if cross else {})
        return remote(
            mine_h.at[q, his if cross else mine], hid.at[q, s, :, units],
            d_send.at[q, s, cross], d_recv.at[q, s, cross], target,
        )

    def d_arrival(q, s, cross):
        there = pl.ds(pl.multiple_of((1 - core) * chunk, chunk), chunk) if cross else units
        return remote(mine_h.at[q, mine], hid.at[q, s, :, there], d_send.at[q, s, cross], d_recv.at[q, s, cross], other_y)

    def d_relay(q, dx):
        s = dx * 2 + 1
        return remote(hid.at[q, 1], hid.at[q, s], d_send.at[q, s, 0], d_recv.at[q, s, 0], to_row(dx, 0))

    d_out = []

    def block_end(q):
        gate, upper = pair_sum(q, 0)
        for dx in (2, 1, 3):
            x_copy(q, dx).wait_recv()
            gate = gate + xrecv[q, dx - 1, :, :chunk].astype(F32)
            upper = upper + xrecv[q, dx - 1, :, chunk:].astype(F32)
        mine_h[q] = (silu(gate) * upper).astype(BF16)
        hid[q, 0, :, units] = mine_h[q, mine, :]
        for s in (1, 2, 6, 4, 0):
            for cross in (0, 1):
                if s or cross:
                    copy = d_copy(q, s, cross)
                    copy.start()
                    d_out.append(copy)

    def block_relay(q):
        for cross in (0, 1):
            d_arrival(q, 1, cross).wait_recv()
        for dx in (1, 3, 2):
            copy = d_relay(q, dx)
            copy.start()
            d_out.append(copy)

    block_end(0)
    y_start(1, 3)
    y_start(1, 0)
    pair_send(1, 2)

    def result_part(dx, dy):
        target = ahead(4 - dx) * 2 + lax.rem(yl + dy, 2)
        return dot(hid_e[...], wd[:, pl.ds(pl.multiple_of(target * width, 128), width)])

    def ey_copy(dx):
        return remote(eysend.at[dx], eyrecv.at[dx], ey_send.at[dx], ey_recv.at[dx], other_y)

    def ex_copy(dx):
        return remote(exsend.at[dx - 1], exrecv.at[dx - 1], ex_send.at[dx - 1], ex_recv.at[dx - 1], {"x": ahead(4 - dx)})

    def result_start(dx):
        eysend[dx] = result_part(dx, 1).astype(BF16)
        ey_copy(dx).start()

    def result_sum(dx):
        ey_copy(dx).wait_recv()
        return result_part(dx, 0) + eyrecv[dx].astype(F32)

    loads[5].wait()
    for dx in (2, 1, 3):
        result_start(dx)
    pair_send(1, 1)
    block_relay(0)
    pair_send(1, 3)
    block_end(1)
    result_start(0)
    for dx in (2, 1, 3):
        exsend[dx - 1] = result_sum(dx).astype(BF16)
        ex_copy(dx).start()
    block_relay(1)
    total = result_sum(0)
    for dx in (2, 1, 3):
        ex_copy(dx).wait_recv()
        total = total + exrecv[dx - 1].astype(F32)
    high = total.astype(BF16)
    hilo[:slots] = high
    hilo[slots : 2 * slots] = (total - high.astype(F32)).astype(BF16)
    k_copy = remote(hilo.at[: 2 * slots], hilo.at[2 * slots :], k_send, k_recv, sibling)
    k_copy.start()
    for q in (0, 1):
        loads[6 + q].wait()
        w_out[q].wait_recv()
        d_arrival(q, 0, 1).wait_recv()
    k_copy.wait_recv()

    def f_copy(s, q):
        target = {"yh": lax.rem(yh + q // 4, 2), "z": lax.rem(z + q % 4, 4)}
        return remote(fsend.at[s], frecv.at[q - 1], f_send.at[q - 1], f_recv.at[q - 1], target)

    def finish(s):
        j = owner(s)
        tokens_of = pl.ds(pl.multiple_of(j * block + core * half, half), half)
        total = dot(hid[0, s], sd[0]) + dot(hid[1, s], sd[1]) + dot(place[tokens_of, :], hilo[...])
        q = lax.rem(j // 4 + yh, 2) * 4 + lax.rem(lax.rem(j, 4) + 4 - z, 4)

        @pl.when(q == 0)
        def _():
            own[...] = total

        @pl.when(q > 0)
        def _():
            fsend[s] = total.astype(BF16)
            f_copy(s, q).start()

    for s in (0, 1, 2, 6, 4, 3, 7, 5):
        for q in (0, 1):
            if s in (2, 4, 6):
                d_arrival(q, s, 0).wait_recv()
                d_arrival(q, s, 1).wait_recv()
            elif s > 1:
                d_relay(q, s // 2).wait_recv()
        finish(s)

    total = own[...]
    for q in range(1, ROWS):
        f_copy(0, q).wait_recv()
        total = total + frecv[q - 1].astype(F32)
    out[...] = total.astype(BF16)

    for s in order:
        a_copy(s).wait_send()
        s_copy(s).wait_send()
    for dx in range(4):
        y_copy(0, dx).wait_send()
        y_copy(1, dx).wait_send()
        ey_copy(dx).wait_send()
    for dx in (1, 2, 3):
        x_copy(0, dx).wait_send()
        x_copy(1, dx).wait_send()
        ex_copy(dx).wait_send()
    for copy in b_out + d_out + w_out + [k_copy]:
        copy.wait_send()
    for q in range(1, ROWS):
        f_copy(0, q).wait_send()


def per_device(tokens, expert_ids, modality, tile_counts, router, w_gate, w_up, w_down, shared_gate, shared_up, shared_down):
    block, depth = tokens.shape
    width = shared_down.shape[1]
    hidden = shared_gate.shape[1]
    inner = w_gate.shape[2]
    slots = 2 * MAXT * TILE
    half = block // 2
    chunk = hidden // 2
    count = expert_ids.shape[0]
    vmem = pl.BlockSpec(memory_space=pltpu.VMEM)
    hbm = pl.BlockSpec(memory_space=pl.ANY)
    dma = pltpu.SemaphoreType.DMA
    return pl.pallas_call(
        kernel,
        name="layer",
        out_shape=jax.ShapeDtypeStruct((half, width), BF16),
        in_specs=[vmem, vmem, pl.BlockSpec(memory_space=pltpu.SMEM), hbm, vmem] + [hbm] * 6,
        out_specs=vmem,
        scratch_shapes=[
            pltpu.VMEM((depth, inner), BF16),
            pltpu.VMEM((depth, inner), BF16),
            pltpu.VMEM((inner, depth), BF16),
            pltpu.VMEM((width, hidden), BF16),
            pltpu.VMEM((width, hidden), BF16),
            pltpu.VMEM((2, 2 * chunk, width), BF16),
            pltpu.VMEM((ROWS, block, width), BF16),
            pltpu.VMEM((slots, count), BF16),
            pltpu.VMEM((count, 4 * slots), BF16),
            pltpu.VMEM((2, 4, block, 2 * chunk), BF16),
            pltpu.VMEM((2, 4, block, 2 * chunk), BF16),
            pltpu.VMEM((2, 3, block, 2 * chunk), BF16),
            pltpu.VMEM((2, 3, block, 2 * chunk), BF16),
            pltpu.VMEM((ROWS, slots, width), BF16),
            pltpu.VMEM((slots, inner), BF16),
            pltpu.VMEM((4, slots, width), BF16),
            pltpu.VMEM((4, slots, width), BF16),
            pltpu.VMEM((3, slots, width), BF16),
            pltpu.VMEM((3, slots, width), BF16),
            pltpu.VMEM((4 * slots, width), BF16),
            pltpu.VMEM((2, block, chunk), BF16),
            pltpu.VMEM((2, ROWS, half, 2 * chunk), BF16),
            pltpu.VMEM((half, width), F32),
            pltpu.VMEM((ROWS, half, width), BF16),
            pltpu.VMEM((ROWS - 1, half, width), BF16),
            dma((8,)),
            dma((ROWS,)), dma((ROWS,)), dma((ROWS,)), dma((ROWS,)),
            dma((2, 4)), dma((2, 4)), dma((2, 3)), dma((2, 3)),
            dma((ROWS,)), dma((ROWS,)),
            dma((4,)), dma((4,)), dma((3,)), dma((3,)),
            dma((2, ROWS, 2)), dma((2, ROWS, 2)), dma((2,)), dma((2,)), dma, dma, dma((ROWS - 1,)), dma((ROWS - 1,)),
        ],
        compiler_params=pltpu.CompilerParams(
            collective_id=0, has_side_effects=True, vmem_limit_bytes=60 * 1024 * 1024
        ),
    )(
        expert_ids.reshape(1, count), modality.reshape(1, count), tile_counts, tokens, router.reshape(1, depth),
        w_gate, w_up, w_down, shared_gate, shared_up, shared_down,
    )


def solution(mesh):
    split = Mesh(mesh.devices.reshape(4, 2, 2, 4, 2), ("x", "yl", "yh", "z", "core"))
    placed = (
        P(ROW, None),
        P(),
        P(),
        P(),
        P(None, COL),
        P(COL, None, ROW),
        P(COL, None, ROW),
        P(COL, ROW, None),
        P(ROW, COL),
        P(ROW, COL),
        P(COL, ROW),
    )
    return jax.shard_map(
        per_device, mesh=split, in_specs=placed, out_specs=P(COL, ROW), check_vma=False
    )
```

```python
import jax
import jax.numpy as jnp
from jax import lax
from jax.experimental import pallas as pl
from jax.experimental.pallas import tpu as pltpu
from jax.sharding import Mesh
from jax.sharding import PartitionSpec as P

TILE = 8
MAXT = 4
ROW = ("x", "yl")
COL = ("yh", "z", "core")
ROWS = 8
MESH = pl.DeviceIdType.MESH
BF16 = jnp.bfloat16
F32 = jnp.float32


def dot(a, b):
    return jnp.dot(a, b, preferred_element_type=F32)


def silu(v):
    return v / (1.0 + jnp.exp(-v))


def kernel(
    ids, mod, counts, tokens, router, w_gate, w_up, w_down, s_gate, s_up, s_down,
    out,
    rows_in, wg, wu, wd, sg, su, sd0, sd1, xs, table, place,
    ysend0, ysend1, yrecv0, yrecv1, xsend0, xsend1, xrecv0, xrecv1, taken,
    hid_e, eysend, eyrecv, exsend, exrecv, efar, egot, hilo, mine_h0, mine_h1, hid0, hid1, early, own, fsend, frecv,
    load_sem, a_send, a_recv, s_send, s_recv, y_send, y_recv, x_send, x_recv, b_send, b_recv,
    ey_send, ey_recv, ex_send, ex_recv, ef_send, ef_recv, d_send, d_recv, w_send, w_recv, k_send, k_recv, f_send, f_recv,
):
    x, yl, yh = lax.axis_index("x"), lax.axis_index("yl"), lax.axis_index("yh")
    z, core = lax.axis_index("z"), lax.axis_index("core")
    block, width = xs.shape[1], xs.shape[2]
    half = block // 2
    slots = table.shape[0]
    sd, mine_h, hid = (sd0, sd1), (mine_h0, mine_h1), (hid0, hid1)
    ysend, yrecv, xsend, xrecv = (ysend0, ysend1), (yrecv0, yrecv1), (xsend0, xsend1), (xrecv0, xrecv1)
    sizes = (mine_h0.shape[1], mine_h1.shape[1])
    spans = (slice(0, sizes[0]), slice(sizes[0], sizes[0] + sizes[1]))
    row = x * 2 + yl
    expert = yh * 8 + z * 2 + core

    def ahead(dx):
        return lax.rem(x + dx, 4)

    def owner(slot):
        dx, dy = slot // 2, slot % 2
        return lax.rem(x + 4 - dx, 4) * 2 + (yl + dy) % 2

    def to_row(dx, dy):
        return {"x": ahead(dx), "yl": lax.rem(yl + dy, 2)}

    sibling = {"core": 1 - core}
    other_y = {"yl": 1 - yl}

    def remote(src, dst, send, recv, device):
        return pltpu.make_async_remote_copy(
            src_ref=src, dst_ref=dst, send_sem=send, recv_sem=recv, device_id=device, device_id_type=MESH
        )

    def units(q, of):
        return pl.ds(pl.multiple_of(of * sizes[q], 128), sizes[q])

    loads = [
        pltpu.make_async_copy(tokens, rows_in, load_sem.at[0]),
        pltpu.make_async_copy(tokens.at[:, pl.ds(pl.multiple_of(row * width, 128), width)], xs.at[0], load_sem.at[9]),
        pltpu.make_async_copy(s_gate, sg, load_sem.at[1]),
        pltpu.make_async_copy(s_up, su, load_sem.at[2]),
        pltpu.make_async_copy(w_gate.at[0], wg, load_sem.at[3]),
        pltpu.make_async_copy(w_up.at[0], wu, load_sem.at[4]),
        pltpu.make_async_copy(w_down.at[0], wd, load_sem.at[5]),
        pltpu.make_async_copy(s_down.at[spans[0]], sd[0].at[units(0, core)], load_sem.at[6]),
        pltpu.make_async_copy(s_down.at[spans[1]], sd[1].at[units(1, core)], load_sem.at[7]),
    ]
    for load in loads:
        load.start()

    barrier = pltpu.get_barrier_semaphore()
    peers = [to_row(s // 2, s % 2) for s in range(1, ROWS)]
    peers += [to_row(s // 2, s % 2) | sibling for s in (1, 2, 4, 6)] + [sibling]
    peers += [{"yh": lax.rem(yh + q // 4, 2), "z": lax.rem(z + q % 4, 4)} for q in range(1, 8)]
    for peer in peers:
        pl.semaphore_signal(barrier, inc=1, device_id=peer, device_id_type=MESH)

    count = ids.shape[1]
    lane = lax.broadcasted_iota(jnp.int32, (2, count), 1)
    kind = lax.broadcasted_iota(jnp.int32, (2, count), 0)
    at = lax.broadcasted_iota(jnp.int32, (slots, count), 0)

    def ones_of(expert):
        member = (ids[...] == expert) & (mod[...] == kind)
        rank = member.astype(jnp.int32)
        step = 1
        while step < count:
            rank = rank + jnp.where(lane >= step, pltpu.roll(rank, step, 1), 0)
            step *= 2
        rank = rank - 1
        limit = jnp.where(kind == 0, counts[0, expert], counts[1, expert]) * TILE
        spot = jnp.where(member & (rank < limit), kind * (MAXT * TILE) + rank, -1)
        return (at == jnp.maximum(spot[0:1, :], spot[1:2, :])).astype(F32)

    ones = ones_of(expert)
    table[...] = ones.astype(BF16)
    place[:, : 2 * slots] = jnp.concatenate([ones, ones], axis=0).T.astype(BF16)

    pl.semaphore_wait(barrier, len(peers))

    mine = pl.ds(pl.multiple_of(core * half, half), half)
    his = pl.ds(pl.multiple_of((1 - core) * half, half), half)

    def a_copy(s):
        dx, dy = s // 2, s % 2
        target = ahead(dx) * 2 + lax.rem(yl + dy, 2)
        return remote(
            rows_in.at[mine, pl.ds(pl.multiple_of(target * width, 128), width)],
            xs.at[s, mine], a_send.at[s], a_recv.at[s], to_row(dx, dy),
        )

    def s_copy(s):
        return remote(xs.at[s, mine], xs.at[s, mine], s_send.at[s], s_recv.at[s], sibling)

    def s_arrival(s):
        return remote(xs.at[s, his], xs.at[s, his], s_send.at[s], s_recv.at[s], sibling)

    order = (5, 3, 7, 1, 4, 2, 6)
    loads[0].wait()
    for s in order:
        a_copy(s).start()

    def y_copy(q, dx):
        return remote(ysend[q].at[dx], yrecv[q].at[dx], y_send.at[q, dx], y_recv.at[q, dx], other_y)

    def x_copy(q, dx):
        return remote(
            xsend[q].at[dx - 1], xrecv[q].at[dx - 1], x_send.at[q, dx - 1], x_recv.at[q, dx - 1], {"x": ahead(4 - dx)}
        )

    w_out = [
        remote(s_down.at[spans[q]], sd[q].at[units(q, core)], w_send.at[q], w_recv.at[q], sibling)
        for q in (0, 1)
    ]
    for copy in w_out:
        copy.start()
    ones = ones_of(yh * 8 + z * 2 + 1 - core)
    place[:, 2 * slots :] = jnp.concatenate([ones, ones], axis=0).T.astype(BF16)

    def part(q, s):
        return dot(xs[s], sg[:, spans[q]]), dot(xs[s], su[:, spans[q]])

    def y_start(q, dx):
        gate, upper = part(q, dx * 2 + 1)
        ysend[q][dx, :, : sizes[q]] = gate.astype(BF16)
        ysend[q][dx, :, sizes[q] :] = upper.astype(BF16)
        y_copy(q, dx).start()

    for load in loads[1:4]:
        load.wait()
    for s in order[:2]:
        a_copy(s).wait_recv()
        s_copy(s).start()
    s_arrival(order[0]).wait_recv()
    y_start(0, 2)
    for s in order[2:]:
        a_copy(s).wait_recv()
        s_copy(s).start()

    def part_of(s):
        columns = pl.ds(pl.multiple_of(owner(s) * block, 128), block)
        return dot(table[:, columns], xs[s])

    rows = part_of(0)
    for i, s in enumerate(order):
        if i > 0:
            s_arrival(s).wait_recv()
        rows = rows + part_of(s)
    taken[0] = rows.astype(BF16)

    def b_copy(source, dx, dy):
        s = dx * 2 + dy if source == 0 else dx * 2 + 1
        return remote(taken.at[source], taken.at[s], b_send.at[s], b_recv.at[s], to_row(dx, dy))

    def b_arrival(s):
        return remote(taken.at[s], taken.at[s], b_send.at[s], b_recv.at[s], other_y)

    b_out = [b_copy(0, 0, 1), b_copy(0, 2, 0), b_copy(0, 1, 0), b_copy(0, 3, 0)]
    for copy in b_out:
        copy.start()

    for q, dx in ((0, 1), (0, 3), (0, 0), (1, 2), (1, 1), (1, 3)):
        y_start(q, dx)

    def pair_sum(q, dx):
        y_copy(q, dx).wait_recv()
        gate, upper = part(q, dx * 2)
        return gate + yrecv[q][dx, :, : sizes[q]].astype(F32), upper + yrecv[q][dx, :, sizes[q] :].astype(F32)

    def pair_send(q, dx):
        gate, upper = pair_sum(q, dx)
        xsend[q][dx - 1, :, : sizes[q]] = gate.astype(BF16)
        xsend[q][dx - 1, :, sizes[q] :] = upper.astype(BF16)
        x_copy(q, dx).start()

    b_arrival(1).wait_recv()
    relayed = [b_copy(1, dx, 0) for dx in (2, 1, 3)]
    for copy in relayed:
        copy.start()
    b_out += relayed
    for dx in (2, 1, 3):
        pair_send(0, dx)

    for s in (2, 3, 4, 5, 6, 7):
        b_arrival(s).wait_recv()
    loads[4].wait()
    loads[5].wait()

    def score_part(s, total):
        line = router[:, pl.ds(pl.multiple_of(owner(s) * width, 128), width)].astype(F32)
        return total + jnp.sum(taken[s].astype(F32) * line, axis=1, keepdims=True)

    logit = lax.fori_loop(0, ROWS, score_part, jnp.zeros((slots, 1), F32))
    score = 1.0 / (1.0 + jnp.exp(-logit))

    def expert_part(s, sums):
        gate, upper = sums
        scaled = (taken[s].astype(F32) * score).astype(BF16)
        features = pl.ds(pl.multiple_of(owner(s) * width, 128), width)
        return gate + dot(scaled, wg[features, :]), upper + dot(scaled, wu[features, :])

    zero = jnp.zeros((slots, wg.shape[1]), F32)
    gate, upper = lax.fori_loop(0, ROWS, expert_part, (zero, zero))
    hid_e[...] = (silu(gate) * upper).astype(BF16)

    def d_copy(q, s, cross):
        target = to_row(s // 2, s % 2) | ({"core": 1 - core} if cross else {})
        return remote(
            mine_h[q].at[his if cross else mine], hid[q].at[s, :, units(q, core)],
            d_send.at[q, s, cross], d_recv.at[q, s, cross], target,
        )

    def d_arrival(q, s, cross):
        there = units(q, 1 - core if cross else core)
        return remote(mine_h[q].at[mine], hid[q].at[s, :, there], d_send.at[q, s, cross], d_recv.at[q, s, cross], other_y)

    def d_relay(q, dx):
        s = dx * 2 + 1
        return remote(hid[q].at[1], hid[q].at[s], d_send.at[q, s, 0], d_recv.at[q, s, 0], to_row(dx, 0))

    d_out = []

    def block_end(q):
        gate, upper = pair_sum(q, 0)
        for dx in (2, 1, 3):
            x_copy(q, dx).wait_recv()
            gate = gate + xrecv[q][dx - 1, :, : sizes[q]].astype(F32)
            upper = upper + xrecv[q][dx - 1, :, sizes[q] :].astype(F32)
        mine_h[q][...] = (silu(gate) * upper).astype(BF16)
        hid[q][0, :, units(q, core)] = mine_h[q][mine, :]
        for s in (1, 2, 6, 4, 0):
            for cross in (0, 1):
                if s or cross:
                    copy = d_copy(q, s, cross)
                    copy.start()
                    d_out.append(copy)

    def block_relay(q):
        for cross in (0, 1):
            d_arrival(q, 1, cross).wait_recv()
        for dx in (1, 3, 2):
            copy = d_relay(q, dx)
            copy.start()
            d_out.append(copy)

    def result_part(dx, dy):
        target = ahead(4 - dx) * 2 + lax.rem(yl + dy, 2)
        return dot(hid_e[...], wd[:, pl.ds(pl.multiple_of(target * width, 128), width)])

    def ey_copy(dx):
        return remote(eysend.at[dx], eyrecv.at[dx], ey_send.at[dx], ey_recv.at[dx], other_y)

    def ex_copy(dx):
        return remote(exsend.at[dx], exrecv.at[dx], ex_send.at[dx], ex_recv.at[dx], {"x": ahead(4 - dx)})

    far_copy = remote(efar, egot, ef_send, ef_recv, {"x": ahead(2)})

    loads[6].wait()
    efar[0] = result_part(2, 0).astype(BF16)
    efar[1] = result_part(2, 1).astype(BF16)
    far_copy.start()
    for dx in (1, 3):
        eysend[dx] = result_part(dx, 1).astype(BF16)
        ey_copy(dx).start()
    y_start(1, 0)
    for dx in (2, 1, 3):
        pair_send(1, dx)
    far_copy.wait_recv()
    eysend[0] = (result_part(0, 1) + egot[1].astype(F32)).astype(BF16)
    ey_copy(0).start()
    for dx in (1, 3):
        ey_copy(dx).wait_recv()
        exsend[dx] = (result_part(dx, 0) + eyrecv[dx].astype(F32)).astype(BF16)
        ex_copy(dx).start()
    block_end(0)
    total = result_part(0, 0) + egot[0].astype(F32)
    block_end(1)
    block_relay(0)
    ey_copy(0).wait_recv()
    total = total + eyrecv[0].astype(F32)
    for dx in (1, 3):
        ex_copy(dx).wait_recv()
        total = total + exrecv[dx].astype(F32)
    high = total.astype(BF16)
    hilo[:slots] = high
    hilo[slots : 2 * slots] = (total - high.astype(F32)).astype(BF16)
    k_copy = remote(hilo.at[: 2 * slots], hilo.at[2 * slots :], k_send, k_recv, sibling)
    k_copy.start()
    for q in (0, 1):
        loads[7 + q].wait()
        w_out[q].wait_recv()
        d_arrival(q, 0, 1).wait_recv()

    def f_copy(s, q):
        target = {"yh": lax.rem(yh + q // 4, 2), "z": lax.rem(z + q % 4, 4)}
        return remote(fsend.at[s], frecv.at[q - 1], f_send.at[q - 1], f_recv.at[q - 1], target)

    def begin(s):
        tokens_of = pl.ds(pl.multiple_of(owner(s) * block + core * half, half), half)
        return dot(hid[0][s], sd[0][...]) + dot(place[tokens_of, :], hilo[...])

    def finish(s, begun=None):
        j = owner(s)
        total = (begin(s) if begun is None else begun) + dot(hid[1][s], sd[1][...])
        q = lax.rem(j // 4 + yh, 2) * 4 + lax.rem(lax.rem(j, 4) + 4 - z, 4)

        @pl.when(q == 0)
        def _():
            own[...] = total

        @pl.when(q > 0)
        def _():
            fsend[s] = total.astype(BF16)
            f_copy(s, q).start()

    def arrive(s):
        for q in (0, 1):
            d_arrival(q, s, 0).wait_recv()
            d_arrival(q, s, 1).wait_recv()

    block_relay(1)
    k_copy.wait_recv()
    finish(0)
    finish(1)
    for s in (2, 6, 4):
        arrive(s)
        finish(s)
    for dx in (1, 3, 2):
        d_relay(0, dx).wait_recv()
        early[dx - 1] = begin(dx * 2 + 1)
    for dx in (1, 3, 2):
        d_relay(1, dx).wait_recv()
        finish(dx * 2 + 1, early[dx - 1])

    total = own[...]
    for q in range(1, ROWS):
        f_copy(0, q).wait_recv()
        total = total + frecv[q - 1].astype(F32)
    out[...] = total.astype(BF16)

    for s in order:
        a_copy(s).wait_send()
        s_copy(s).wait_send()
    for dx in range(4):
        y_copy(0, dx).wait_send()
        y_copy(1, dx).wait_send()
    for dx in (1, 2, 3):
        x_copy(0, dx).wait_send()
        x_copy(1, dx).wait_send()
    e_out = [ey_copy(0), ey_copy(1), ey_copy(3), ex_copy(1), ex_copy(3), far_copy]
    for copy in b_out + d_out + e_out + w_out + [k_copy]:
        copy.wait_send()
    for q in range(1, ROWS):
        f_copy(0, q).wait_send()


def per_device(tokens, expert_ids, modality, tile_counts, router, w_gate, w_up, w_down, shared_gate, shared_up, shared_down):
    block, depth = tokens.shape
    width = shared_down.shape[1]
    hidden = shared_gate.shape[1]
    inner = w_gate.shape[2]
    slots = 2 * MAXT * TILE
    half = block // 2
    sizes = (256, hidden - 256)
    count = expert_ids.shape[0]
    vmem = pl.BlockSpec(memory_space=pltpu.VMEM)
    hbm = pl.BlockSpec(memory_space=pl.ANY)
    dma = pltpu.SemaphoreType.DMA
    return pl.pallas_call(
        kernel,
        name="layer",
        out_shape=jax.ShapeDtypeStruct((half, width), BF16),
        in_specs=[vmem, vmem, pl.BlockSpec(memory_space=pltpu.SMEM), hbm, vmem] + [hbm] * 6,
        out_specs=vmem,
        scratch_shapes=[
            pltpu.VMEM((block, depth), BF16),
            pltpu.VMEM((depth, inner), BF16),
            pltpu.VMEM((depth, inner), BF16),
            pltpu.VMEM((inner, depth), BF16),
            pltpu.VMEM((width, hidden), BF16),
            pltpu.VMEM((width, hidden), BF16),
            *(pltpu.VMEM((2 * size, width), BF16) for size in sizes),
            pltpu.VMEM((ROWS, block, width), BF16),
            pltpu.VMEM((slots, count), BF16),
            pltpu.VMEM((count, 4 * slots), BF16),
            *(pltpu.VMEM((4, block, 2 * size), BF16) for size in sizes + sizes),
            *(pltpu.VMEM((3, block, 2 * size), BF16) for size in sizes + sizes),
            pltpu.VMEM((ROWS, slots, width), BF16),
            pltpu.VMEM((slots, inner), BF16),
            pltpu.VMEM((4, slots, width), BF16),
            pltpu.VMEM((4, slots, width), BF16),
            pltpu.VMEM((4, slots, width), BF16),
            pltpu.VMEM((4, slots, width), BF16),
            pltpu.VMEM((2, slots, width), BF16),
            pltpu.VMEM((2, slots, width), BF16),
            pltpu.VMEM((4 * slots, width), BF16),
            *(pltpu.VMEM((block, size), BF16) for size in sizes),
            *(pltpu.VMEM((ROWS, half, 2 * size), BF16) for size in sizes),
            pltpu.VMEM((3, half, width), F32),
            pltpu.VMEM((half, width), F32),
            pltpu.VMEM((ROWS, half, width), BF16),
            pltpu.VMEM((ROWS - 1, half, width), BF16),
            dma((10,)),
            dma((ROWS,)), dma((ROWS,)), dma((ROWS,)), dma((ROWS,)),
            dma((2, 4)), dma((2, 4)), dma((2, 3)), dma((2, 3)),
            dma((ROWS,)), dma((ROWS,)),
            dma((4,)), dma((4,)), dma((4,)), dma((4,)), dma, dma,
            dma((2, ROWS, 2)), dma((2, ROWS, 2)), dma((2,)), dma((2,)), dma, dma, dma((ROWS - 1,)), dma((ROWS - 1,)),
        ],
        compiler_params=pltpu.CompilerParams(
            collective_id=0, has_side_effects=True, vmem_limit_bytes=60 * 1024 * 1024
        ),
    )(
        expert_ids.reshape(1, count), modality.reshape(1, count), tile_counts, tokens, router.reshape(1, depth),
        w_gate, w_up, w_down, shared_gate, shared_up, shared_down,
    )


def solution(mesh):
    split = Mesh(mesh.devices.reshape(4, 2, 2, 4, 2), ("x", "yl", "yh", "z", "core"))
    placed = (
        P(ROW, None),
        P(),
        P(),
        P(),
        P(None, COL),
        P(COL, None, ROW),
        P(COL, None, ROW),
        P(COL, ROW, None),
        P(ROW, COL),
        P(ROW, COL),
        P(COL, ROW),
    )
    return jax.shard_map(
        per_device, mesh=split, in_specs=placed, out_specs=P(COL, ROW), check_vma=False
    )
```

```python
import jax
import jax.numpy as jnp
from jax import lax
from jax.experimental import pallas as pl
from jax.experimental.pallas import tpu as pltpu
from jax.sharding import Mesh
from jax.sharding import PartitionSpec as P

TILE = 8
MAXT = 4
ROW = ("x", "yl")
COL = ("yh", "z", "core")
ROWS = 8
MESH = pl.DeviceIdType.MESH
BF16 = jnp.bfloat16
F32 = jnp.float32


def dot(a, b):
    return jnp.dot(a, b, preferred_element_type=F32)


def silu(v):
    return v / (1.0 + jnp.exp(-v))


def kernel(
    ids, mod, counts, tokens, router, w_gate, w_up, w_down, s_gate, s_up, s_down,
    out,
    rows_in, wg, wu, wd, sg, su, sd0, sd1, xs, table, place,
    ysend0, ysend1, yrecv0, yrecv1, xsend0, xsend1, xrecv0, xrecv1, taken,
    hid_e, eysend, eyrecv, exsend, exrecv, efar, egot, hilo, mine_h0, mine_h1, hid0, hid1, early, own, fsend, frecv,
    load_sem, a_send, a_recv, s_send, s_recv, y_send, y_recv, x_send, x_recv, b_send, b_recv,
    ey_send, ey_recv, ex_send, ex_recv, ef_send, ef_recv, d_send, d_recv, w_send, w_recv, k_send, k_recv, f_send, f_recv,
):
    x, yl, yh = lax.axis_index("x"), lax.axis_index("yl"), lax.axis_index("yh")
    z, core = lax.axis_index("z"), lax.axis_index("core")
    block, width = xs.shape[1], xs.shape[2]
    half = block // 2
    slots = table.shape[0]
    sd, mine_h, hid = (sd0, sd1), (mine_h0, mine_h1), (hid0, hid1)
    ysend, yrecv, xsend, xrecv = (ysend0, ysend1), (yrecv0, yrecv1), (xsend0, xsend1), (xrecv0, xrecv1)
    sizes = (mine_h0.shape[1], mine_h1.shape[1])
    spans = (slice(0, sizes[0]), slice(sizes[0], sizes[0] + sizes[1]))
    row = x * 2 + yl
    expert = yh * 8 + z * 2 + core

    def ahead(dx):
        return lax.rem(x + dx, 4)

    def owner(slot):
        dx, dy = slot // 2, slot % 2
        return lax.rem(x + 4 - dx, 4) * 2 + (yl + dy) % 2

    def to_row(dx, dy):
        return {"x": ahead(dx), "yl": lax.rem(yl + dy, 2)}

    sibling = {"core": 1 - core}
    other_y = {"yl": 1 - yl}

    def remote(src, dst, send, recv, device):
        return pltpu.make_async_remote_copy(
            src_ref=src, dst_ref=dst, send_sem=send, recv_sem=recv, device_id=device, device_id_type=MESH
        )

    def units(q, of):
        return pl.ds(pl.multiple_of(of * sizes[q], 128), sizes[q])

    loads = [
        pltpu.make_async_copy(tokens, rows_in, load_sem.at[0]),
        pltpu.make_async_copy(tokens.at[:, pl.ds(pl.multiple_of(row * width, 128), width)], xs.at[0], load_sem.at[9]),
        pltpu.make_async_copy(s_gate, sg, load_sem.at[1]),
        pltpu.make_async_copy(s_up, su, load_sem.at[2]),
        pltpu.make_async_copy(w_gate.at[0], wg, load_sem.at[3]),
        pltpu.make_async_copy(w_up.at[0], wu, load_sem.at[4]),
        pltpu.make_async_copy(w_down.at[0], wd, load_sem.at[5]),
        pltpu.make_async_copy(s_down.at[spans[0]], sd[0].at[units(0, core)], load_sem.at[6]),
        pltpu.make_async_copy(s_down.at[spans[1]], sd[1].at[units(1, core)], load_sem.at[7]),
    ]
    for load in loads:
        load.start()

    barrier = pltpu.get_barrier_semaphore()
    peers = [to_row(s // 2, s % 2) for s in range(1, ROWS)]
    peers += [to_row(s // 2, s % 2) | sibling for s in (1, 2, 4, 6)] + [sibling]
    peers += [{"yh": lax.rem(yh + q // 4, 2), "z": lax.rem(z + q % 4, 4)} for q in range(1, 8)]
    for peer in peers:
        pl.semaphore_signal(barrier, inc=1, device_id=peer, device_id_type=MESH)

    count = ids.shape[1]
    lane = lax.broadcasted_iota(jnp.int32, (2, count), 1)
    kind = lax.broadcasted_iota(jnp.int32, (2, count), 0)
    at = lax.broadcasted_iota(jnp.int32, (slots, count), 0)

    def ones_of(expert):
        member = (ids[...] == expert) & (mod[...] == kind)
        rank = member.astype(jnp.int32)
        step = 1
        while step < count:
            rank = rank + jnp.where(lane >= step, pltpu.roll(rank, step, 1), 0)
            step *= 2
        rank = rank - 1
        limit = jnp.where(kind == 0, counts[0, expert], counts[1, expert]) * TILE
        spot = jnp.where(member & (rank < limit), kind * (MAXT * TILE) + rank, -1)
        return (at == jnp.maximum(spot[0:1, :], spot[1:2, :])).astype(F32)

    pl.semaphore_wait(barrier, len(peers))

    mine = pl.ds(pl.multiple_of(core * half, half), half)
    his = pl.ds(pl.multiple_of((1 - core) * half, half), half)

    def a_copy(s):
        dx, dy = s // 2, s % 2
        target = ahead(dx) * 2 + lax.rem(yl + dy, 2)
        return remote(
            rows_in.at[mine, pl.ds(pl.multiple_of(target * width, 128), width)],
            xs.at[s, mine], a_send, a_recv.at[s], to_row(dx, dy),
        )

    def s_copy(s):
        return remote(xs.at[s, mine], xs.at[s, mine], s_send, s_recv.at[s], sibling)

    def s_arrival(s):
        return remote(xs.at[s, his], xs.at[s, his], s_send, s_recv.at[s], sibling)

    order = (5, 3, 7, 1, 4, 2, 6)
    loads[0].wait()
    for s in order:
        a_copy(s).start()

    def y_copy(q, dx):
        return remote(ysend[q].at[dx], yrecv[q].at[dx], y_send.at[q], y_recv.at[q, dx], other_y)

    def x_copy(q, dx):
        return remote(
            xsend[q].at[dx - 1], xrecv[q].at[dx - 1], x_send.at[q], x_recv.at[q, dx - 1], {"x": ahead(4 - dx)}
        )

    w_out = [
        remote(s_down.at[spans[q]], sd[q].at[units(q, core)], w_send.at[q], w_recv.at[q], sibling)
        for q in (0, 1)
    ]
    for copy in w_out:
        copy.start()
    ones = ones_of(expert)
    table[...] = ones.astype(BF16)
    place[:, : 2 * slots] = jnp.concatenate([ones, ones], axis=0).T.astype(BF16)
    ones = ones_of(yh * 8 + z * 2 + 1 - core)
    place[:, 2 * slots :] = jnp.concatenate([ones, ones], axis=0).T.astype(BF16)

    def part(q, s):
        return dot(xs[s], sg[:, spans[q]]), dot(xs[s], su[:, spans[q]])

    def y_start(q, dx):
        gate, upper = part(q, dx * 2 + 1)
        ysend[q][dx, :, : sizes[q]] = gate.astype(BF16)
        ysend[q][dx, :, sizes[q] :] = upper.astype(BF16)
        y_copy(q, dx).start()

    for load in loads[1:4]:
        load.wait()
    for s in order[:2]:
        a_copy(s).wait_recv()
        s_copy(s).start()
    s_arrival(order[0]).wait_recv()
    y_start(0, 2)
    for s in order[2:]:
        a_copy(s).wait_recv()
        s_copy(s).start()

    def part_of(s):
        columns = pl.ds(pl.multiple_of(owner(s) * block, 128), block)
        return dot(table[:, columns], xs[s])

    rows = part_of(0)
    for i, s in enumerate(order):
        if i > 0:
            s_arrival(s).wait_recv()
        rows = rows + part_of(s)
    taken[0] = rows.astype(BF16)

    def b_copy(source, dx, dy):
        s = dx * 2 + dy if source == 0 else dx * 2 + 1
        return remote(taken.at[source], taken.at[s], b_send, b_recv.at[s], to_row(dx, dy))

    def b_arrival(s):
        return remote(taken.at[s], taken.at[s], b_send, b_recv.at[s], other_y)

    b_out = [b_copy(0, 0, 1), b_copy(0, 2, 0), b_copy(0, 1, 0), b_copy(0, 3, 0)]
    for copy in b_out:
        copy.start()

    for q, dx in ((0, 1), (0, 3), (0, 0), (1, 2), (1, 1), (1, 3)):
        y_start(q, dx)

    def pair_sum(q, dx):
        y_copy(q, dx).wait_recv()
        gate, upper = part(q, dx * 2)
        return gate + yrecv[q][dx, :, : sizes[q]].astype(F32), upper + yrecv[q][dx, :, sizes[q] :].astype(F32)

    def pair_send(q, dx):
        gate, upper = pair_sum(q, dx)
        xsend[q][dx - 1, :, : sizes[q]] = gate.astype(BF16)
        xsend[q][dx - 1, :, sizes[q] :] = upper.astype(BF16)
        x_copy(q, dx).start()

    b_arrival(1).wait_recv()
    relayed = [b_copy(1, dx, 0) for dx in (2, 1, 3)]
    for copy in relayed:
        copy.start()
    b_out += relayed
    for dx in (2, 1, 3):
        pair_send(0, dx)

    for s in (2, 3, 4, 5, 6, 7):
        b_arrival(s).wait_recv()
    loads[4].wait()
    loads[5].wait()

    def score_part(s, total):
        line = router[:, pl.ds(pl.multiple_of(owner(s) * width, 128), width)].astype(F32)
        return total + jnp.sum(taken[s].astype(F32) * line, axis=1, keepdims=True)

    logit = lax.fori_loop(0, ROWS, score_part, jnp.zeros((slots, 1), F32))
    score = 1.0 / (1.0 + jnp.exp(-logit))

    def expert_part(s, sums):
        gate, upper = sums
        scaled = (taken[s].astype(F32) * score).astype(BF16)
        features = pl.ds(pl.multiple_of(owner(s) * width, 128), width)
        return gate + dot(scaled, wg[features, :]), upper + dot(scaled, wu[features, :])

    zero = jnp.zeros((slots, wg.shape[1]), F32)
    gate, upper = lax.fori_loop(0, ROWS, expert_part, (zero, zero))
    hid_e[...] = (silu(gate) * upper).astype(BF16)

    def d_copy(q, s, cross):
        target = to_row(s // 2, s % 2) | ({"core": 1 - core} if cross else {})
        return remote(
            mine_h[q].at[his if cross else mine], hid[q].at[s, :, units(q, core)],
            d_send.at[q], d_recv.at[q, s, cross], target,
        )

    def d_arrival(q, s, cross):
        there = units(q, 1 - core if cross else core)
        return remote(mine_h[q].at[mine], hid[q].at[s, :, there], d_send.at[q], d_recv.at[q, s, cross], other_y)

    def d_relay(q, dx):
        s = dx * 2 + 1
        return remote(hid[q].at[1], hid[q].at[s], d_send.at[q], d_recv.at[q, s, 0], to_row(dx, 0))

    def block_end(q):
        gate, upper = pair_sum(q, 0)
        for dx in (2, 1, 3):
            x_copy(q, dx).wait_recv()
            gate = gate + xrecv[q][dx - 1, :, : sizes[q]].astype(F32)
            upper = upper + xrecv[q][dx - 1, :, sizes[q] :].astype(F32)
        mine_h[q][...] = (silu(gate) * upper).astype(BF16)
        hid[q][0, :, units(q, core)] = mine_h[q][mine, :]
        for s in (1, 2, 6, 4, 0):
            for cross in (0, 1):
                if s or cross:
                    copy = d_copy(q, s, cross)
                    copy.start()

    def block_relay(q, steps):
        for cross in (0, 1):
            d_arrival(q, 1, cross).wait_recv()
        for dx in steps:
            copy = d_relay(q, dx)
            copy.start()

    def block_across(q, dx):
        s = dx * 2
        for cross in (0, 1):
            d_arrival(q, s, cross).wait_recv()
        copy = remote(hid[q].at[s], hid[q].at[s + 1], d_send.at[q], d_recv.at[q, s + 1, 0], other_y)
        copy.start()

    def result_part(dx, dy):
        target = ahead(4 - dx) * 2 + lax.rem(yl + dy, 2)
        return dot(hid_e[...], wd[:, pl.ds(pl.multiple_of(target * width, 128), width)])

    def ey_copy(dx):
        return remote(eysend.at[dx], eyrecv.at[dx], ey_send, ey_recv.at[dx], other_y)

    def ex_copy(dx):
        return remote(exsend.at[dx], exrecv.at[dx], ex_send, ex_recv.at[dx], {"x": ahead(4 - dx)})

    far_copy = remote(efar, egot, ef_send, ef_recv, {"x": ahead(2)})

    loads[6].wait()
    efar[0] = result_part(2, 0).astype(BF16)
    efar[1] = result_part(2, 1).astype(BF16)
    far_copy.start()
    for dx in (1, 3):
        eysend[dx] = result_part(dx, 1).astype(BF16)
        ey_copy(dx).start()
    y_start(1, 0)
    for dx in (2, 1, 3):
        pair_send(1, dx)
    far_copy.wait_recv()
    eysend[0] = (result_part(0, 1) + egot[1].astype(F32)).astype(BF16)
    ey_copy(0).start()
    for dx in (1, 3):
        ey_copy(dx).wait_recv()
        exsend[dx] = (result_part(dx, 0) + eyrecv[dx].astype(F32)).astype(BF16)
        ex_copy(dx).start()
    block_end(0)
    total = result_part(0, 0) + egot[0].astype(F32)
    block_end(1)
    block_relay(0, (2,))
    ey_copy(0).wait_recv()
    total = total + eyrecv[0].astype(F32)
    for dx in (1, 3):
        ex_copy(dx).wait_recv()
        total = total + exrecv[dx].astype(F32)
    high = total.astype(BF16)
    hilo[:slots] = high
    hilo[slots : 2 * slots] = (total - high.astype(F32)).astype(BF16)
    k_copy = remote(hilo.at[: 2 * slots], hilo.at[2 * slots :], k_send, k_recv, sibling)
    k_copy.start()
    for q in (0, 1):
        loads[7 + q].wait()
        w_out[q].wait_recv()
        d_arrival(q, 0, 1).wait_recv()

    def f_copy(s, q):
        target = {"yh": lax.rem(yh + q // 4, 2), "z": lax.rem(z + q % 4, 4)}
        return remote(fsend.at[s], frecv.at[q - 1], f_send, f_recv.at[q - 1], target)

    def begin(s):
        tokens_of = pl.ds(pl.multiple_of(owner(s) * block + core * half, half), half)
        return dot(hid[0][s], sd[0][...]) + dot(place[tokens_of, :], hilo[...])

    def finish(s, begun=None):
        j = owner(s)
        total = (begin(s) if begun is None else begun) + dot(hid[1][s], sd[1][...])
        q = lax.rem(j // 4 + yh, 2) * 4 + lax.rem(lax.rem(j, 4) + 4 - z, 4)

        @pl.when(q == 0)
        def _():
            own[...] = total

        @pl.when(q > 0)
        def _():
            fsend[s] = total.astype(BF16)
            f_copy(s, q).start()

    def arrive(s):
        for q in (0, 1):
            if q == 1 or s == 4:
                d_arrival(q, s, 0).wait_recv()
                d_arrival(q, s, 1).wait_recv()

    for dx in (1, 3):
        block_across(0, dx)
    block_relay(1, (1, 3, 2))
    k_copy.wait_recv()
    finish(0)
    finish(1)
    for s in (2, 6, 4):
        arrive(s)
        finish(s)
    for dx in (1, 3, 2):
        d_relay(0, dx).wait_recv()
        early[dx - 1] = begin(dx * 2 + 1)
    for dx in (1, 3, 2):
        d_relay(1, dx).wait_recv()
        finish(dx * 2 + 1, early[dx - 1])

    total = own[...]
    for q in range(1, ROWS):
        f_copy(0, q).wait_recv()
        total = total + frecv[q - 1].astype(F32)
    out[...] = total.astype(BF16)

    def left(bytes_of, sem):
        pltpu.make_async_copy(bytes_of, bytes_of, sem).wait()

    left(frecv, a_send)
    left(frecv, s_send)
    left(frecv, b_send)
    for q in (0, 1):
        left(ysend[q], y_send.at[q])
        left(xsend[q], x_send.at[q])
        left(xs.at[:3, :, : 5 * sizes[q] // 2], d_send.at[q])
        w_out[q].wait_send()
    left(eysend.at[:3], ey_send)
    left(eysend.at[:2], ex_send)
    far_copy.wait_send()
    k_copy.wait_send()
    left(frecv, f_send)


def per_device(tokens, expert_ids, modality, tile_counts, router, w_gate, w_up, w_down, shared_gate, shared_up, shared_down):
    block, depth = tokens.shape
    width = shared_down.shape[1]
    hidden = shared_gate.shape[1]
    inner = w_gate.shape[2]
    slots = 2 * MAXT * TILE
    half = block // 2
    sizes = (256, hidden - 256)
    count = expert_ids.shape[0]
    vmem = pl.BlockSpec(memory_space=pltpu.VMEM)
    hbm = pl.BlockSpec(memory_space=pl.ANY)
    dma = pltpu.SemaphoreType.DMA
    return pl.pallas_call(
        kernel,
        name="layer",
        out_shape=pltpu.VMEM((half, width), BF16),
        in_specs=[vmem, vmem, pl.BlockSpec(memory_space=pltpu.SMEM), hbm, vmem] + [hbm] * 6,
        out_specs=vmem,
        scratch_shapes=[
            pltpu.VMEM((block, depth), BF16),
            pltpu.VMEM((depth, inner), BF16),
            pltpu.VMEM((depth, inner), BF16),
            pltpu.VMEM((inner, depth), BF16),
            pltpu.VMEM((width, hidden), BF16),
            pltpu.VMEM((width, hidden), BF16),
            *(pltpu.VMEM((2 * size, width), BF16) for size in sizes),
            pltpu.VMEM((ROWS, block, width), BF16),
            pltpu.VMEM((slots, count), BF16),
            pltpu.VMEM((count, 4 * slots), BF16),
            *(pltpu.VMEM((4, block, 2 * size), BF16) for size in sizes + sizes),
            *(pltpu.VMEM((3, block, 2 * size), BF16) for size in sizes + sizes),
            pltpu.VMEM((ROWS, slots, width), BF16),
            pltpu.VMEM((slots, inner), BF16),
            pltpu.VMEM((4, slots, width), BF16),
            pltpu.VMEM((4, slots, width), BF16),
            pltpu.VMEM((4, slots, width), BF16),
            pltpu.VMEM((4, slots, width), BF16),
            pltpu.VMEM((2, slots, width), BF16),
            pltpu.VMEM((2, slots, width), BF16),
            pltpu.VMEM((4 * slots, width), BF16),
            *(pltpu.VMEM((block, size), BF16) for size in sizes),
            *(pltpu.VMEM((ROWS, half, 2 * size), BF16) for size in sizes),
            pltpu.VMEM((3, half, width), F32),
            pltpu.VMEM((half, width), F32),
            pltpu.VMEM((ROWS, half, width), BF16),
            pltpu.VMEM((ROWS - 1, half, width), BF16),
            dma((10,)),
            dma, dma((ROWS,)), dma, dma((ROWS,)),
            dma((2,)), dma((2, 4)), dma((2,)), dma((2, 3)),
            dma, dma((ROWS,)),
            dma, dma((4,)), dma, dma((4,)), dma, dma,
            dma((2,)), dma((2, ROWS, 2)), dma((2,)), dma((2,)), dma, dma, dma, dma((ROWS - 1,)),
        ],
        compiler_params=pltpu.CompilerParams(
            collective_id=0, has_side_effects=True, vmem_limit_bytes=60 * 1024 * 1024
        ),
    )(
        expert_ids.reshape(1, count), modality.reshape(1, count), tile_counts, tokens, router.reshape(1, depth),
        w_gate, w_up, w_down, shared_gate, shared_up, shared_down,
    )


def solution(mesh):
    split = Mesh(mesh.devices.reshape(4, 2, 2, 4, 2), ("x", "yl", "yh", "z", "core"))
    placed = (
        P(ROW, None),
        P(),
        P(),
        P(),
        P(None, COL),
        P(COL, None, ROW),
        P(COL, None, ROW),
        P(COL, ROW, None),
        P(ROW, COL),
        P(ROW, COL),
        P(COL, ROW),
    )
    return jax.shard_map(
        per_device, mesh=split, in_specs=placed, out_specs=P(COL, ROW), check_vma=False
    )
```

```python
import jax
import jax.numpy as jnp
from jax import lax
from jax.experimental import pallas as pl
from jax.experimental.pallas import tpu as pltpu
from jax.sharding import Mesh
from jax.sharding import PartitionSpec as P

TILE = 8
MAXT = 4
ROW = ("x", "yl")
COL = ("yh", "z", "core")
ROWS = 8
MESH = pl.DeviceIdType.MESH
BF16 = jnp.bfloat16
F32 = jnp.float32


def dot(a, b):
    return jnp.dot(a, b, preferred_element_type=F32)


def silu(v):
    return v / (1.0 + jnp.exp(-v))


def kernel(
    ids, mod, counts, tokens, router, w_gate, w_up, w_down, s_gate, s_up, s_down,
    out,
    rows_in, wg, wu, wd, sg, su, sd0, sd1, xs, table, place,
    ysend0, ysend1, yrecv0, yrecv1, xsend0, xsend1, xrecv0, xrecv1, taken,
    hid_e, eysend, eyrecv, exsend, exrecv, efar, egot, hilo, mine_h0, mine_h1, hid0, hid1, early, own, fsend, frecv,
    load_sem, a_send, a_recv, s_send, s_recv, y_send, y_recv, x_send, x_recv, b_send, b_recv,
    ey_send, ey_recv, ex_send, ex_recv, ef_send, ef_recv, d_send, d_recv, w_send, w_recv, k_send, k_recv, f_send, f_recv,
):
    x, yl, yh = lax.axis_index("x"), lax.axis_index("yl"), lax.axis_index("yh")
    z, core = lax.axis_index("z"), lax.axis_index("core")
    block, width = xs.shape[1], xs.shape[2]
    half = block // 2
    slots = table.shape[0]
    sd, mine_h, hid = (sd0, sd1), (mine_h0, mine_h1), (hid0, hid1)
    ysend, yrecv, xsend, xrecv = (ysend0, ysend1), (yrecv0, yrecv1), (xsend0, xsend1), (xrecv0, xrecv1)
    sizes = (mine_h0.shape[1], mine_h1.shape[1])
    spans = (slice(0, sizes[0]), slice(sizes[0], sizes[0] + sizes[1]))
    row = x * 2 + yl
    expert = yh * 8 + z * 2 + core

    def ahead(dx):
        return lax.rem(x + dx, 4)

    def owner(slot):
        dx, dy = slot // 2, slot % 2
        return lax.rem(x + 4 - dx, 4) * 2 + (yl + dy) % 2

    def to_row(dx, dy):
        return {"x": ahead(dx), "yl": lax.rem(yl + dy, 2)}

    sibling = {"core": 1 - core}
    other_y = {"yl": 1 - yl}

    def remote(src, dst, send, recv, device):
        return pltpu.make_async_remote_copy(
            src_ref=src, dst_ref=dst, send_sem=send, recv_sem=recv, device_id=device, device_id_type=MESH
        )

    def units(q, of):
        return pl.ds(pl.multiple_of(of * sizes[q], 128), sizes[q])

    loads = [
        pltpu.make_async_copy(tokens, rows_in, load_sem.at[0]),
        pltpu.make_async_copy(tokens.at[:, pl.ds(pl.multiple_of(row * width, 128), width)], xs.at[0], load_sem.at[9]),
        pltpu.make_async_copy(s_gate, sg, load_sem.at[1]),
        pltpu.make_async_copy(s_up, su, load_sem.at[2]),
        pltpu.make_async_copy(w_gate.at[0], wg, load_sem.at[3]),
        pltpu.make_async_copy(w_up.at[0], wu, load_sem.at[4]),
        pltpu.make_async_copy(w_down.at[0], wd, load_sem.at[5]),
        pltpu.make_async_copy(s_down.at[spans[0]], sd[0].at[units(0, core)], load_sem.at[6]),
        pltpu.make_async_copy(s_down.at[spans[1]], sd[1].at[units(1, core)], load_sem.at[7]),
    ]
    for load in loads:
        load.start()

    barrier = pltpu.get_barrier_semaphore()
    peers = [to_row(s // 2, s % 2) for s in range(1, ROWS)]
    peers += [to_row(s // 2, s % 2) | sibling for s in (1, 2, 4, 6)] + [sibling]
    peers += [{"yh": lax.rem(yh + q // 4, 2), "z": lax.rem(z + q % 4, 4)} for q in range(1, 8)]
    for peer in peers:
        pl.semaphore_signal(barrier, inc=1, device_id=peer, device_id_type=MESH)

    count = ids.shape[1]
    lane = lax.broadcasted_iota(jnp.int32, (2, count), 1)
    kind = lax.broadcasted_iota(jnp.int32, (2, count), 0)
    at = lax.broadcasted_iota(jnp.int32, (slots, count), 0)

    def ones_of(expert):
        member = (ids[...] == expert) & (mod[...] == kind)
        rank = member.astype(jnp.int32)
        step = 1
        while step < count:
            rank = rank + jnp.where(lane >= step, pltpu.roll(rank, step, 1), 0)
            step *= 2
        rank = rank - 1
        limit = jnp.where(kind == 0, counts[0, expert], counts[1, expert]) * TILE
        spot = jnp.where(member & (rank < limit), kind * (MAXT * TILE) + rank, -1)
        return (at == jnp.maximum(spot[0:1, :], spot[1:2, :])).astype(F32)

    pl.semaphore_wait(barrier, len(peers))

    mine = pl.ds(pl.multiple_of(core * half, half), half)
    his = pl.ds(pl.multiple_of((1 - core) * half, half), half)

    def a_copy(s):
        dx, dy = s // 2, s % 2
        target = ahead(dx) * 2 + lax.rem(yl + dy, 2)
        return remote(
            rows_in.at[mine, pl.ds(pl.multiple_of(target * width, 128), width)],
            xs.at[s, mine], a_send, a_recv.at[s], to_row(dx, dy),
        )

    def s_copy(s):
        return remote(xs.at[s, mine], xs.at[s, mine], s_send, s_recv.at[s], sibling)

    def s_arrival(s):
        return remote(xs.at[s, his], xs.at[s, his], s_send, s_recv.at[s], sibling)

    order = (5, 3, 7, 1, 4, 2, 6)
    loads[0].wait()
    for s in order:
        a_copy(s).start()

    def y_copy(q, dx):
        return remote(ysend[q].at[dx], yrecv[q].at[dx], y_send.at[q], y_recv.at[q, dx], other_y)

    def x_copy(q, dx):
        return remote(
            xsend[q].at[dx - 1], xrecv[q].at[dx - 1], x_send.at[q], x_recv.at[q, dx - 1], {"x": ahead(4 - dx)}
        )

    w_out = [
        remote(s_down.at[spans[q]], sd[q].at[units(q, core)], w_send.at[q], w_recv.at[q], sibling)
        for q in (0, 1)
    ]
    for copy in w_out:
        copy.start()
    ones = ones_of(expert)
    table[...] = ones.astype(BF16)
    place[:, : 2 * slots] = jnp.concatenate([ones, ones], axis=0).T.astype(BF16)
    ones = ones_of(yh * 8 + z * 2 + 1 - core)
    place[:, 2 * slots :] = jnp.concatenate([ones, ones], axis=0).T.astype(BF16)

    def part(q, s):
        return dot(xs[s], sg[:, spans[q]]), dot(xs[s], su[:, spans[q]])

    def y_start(q, dx):
        gate, upper = part(q, dx * 2 + 1)
        ysend[q][dx, :, : sizes[q]] = gate.astype(BF16)
        ysend[q][dx, :, sizes[q] :] = upper.astype(BF16)
        y_copy(q, dx).start()

    for load in loads[1:4]:
        load.wait()
    for s in order[:2]:
        a_copy(s).wait_recv()
        s_copy(s).start()
    s_arrival(order[0]).wait_recv()
    y_start(0, 2)
    for s in order[2:]:
        a_copy(s).wait_recv()
        s_copy(s).start()

    def part_of(s):
        columns = pl.ds(pl.multiple_of(owner(s) * block, 128), block)
        return dot(table[:, columns], xs[s])

    rows = part_of(0)
    for i, s in enumerate(order):
        if i > 0:
            s_arrival(s).wait_recv()
        rows = rows + part_of(s)
    taken[0] = rows.astype(BF16)

    def b_copy(source, dx, dy):
        s = dx * 2 + dy if source == 0 else dx * 2 + 1
        return remote(taken.at[source], taken.at[s], b_send, b_recv.at[s], to_row(dx, dy))

    def b_arrival(s):
        return remote(taken.at[s], taken.at[s], b_send, b_recv.at[s], other_y)

    b_out = [b_copy(0, 0, 1), b_copy(0, 2, 0), b_copy(0, 1, 0), b_copy(0, 3, 0)]
    for copy in b_out:
        copy.start()

    for q, dx in ((0, 1), (0, 3), (0, 0), (1, 2), (1, 1), (1, 3)):
        y_start(q, dx)

    def pair_sum(q, dx):
        y_copy(q, dx).wait_recv()
        gate, upper = part(q, dx * 2)
        return gate + yrecv[q][dx, :, : sizes[q]].astype(F32), upper + yrecv[q][dx, :, sizes[q] :].astype(F32)

    def pair_send(q, dx):
        gate, upper = pair_sum(q, dx)
        xsend[q][dx - 1, :, : sizes[q]] = gate.astype(BF16)
        xsend[q][dx - 1, :, sizes[q] :] = upper.astype(BF16)
        x_copy(q, dx).start()

    b_arrival(1).wait_recv()
    relayed = [b_copy(1, dx, 0) for dx in (2, 1, 3)]
    for copy in relayed:
        copy.start()
    b_out += relayed
    for dx in (2, 1, 3):
        pair_send(0, dx)

    for s in (2, 3, 4, 5, 6, 7):
        b_arrival(s).wait_recv()
    loads[4].wait()
    loads[5].wait()

    def score_part(s, total):
        line = router[:, pl.ds(pl.multiple_of(owner(s) * width, 128), width)].astype(F32)
        return total + jnp.sum(taken[s].astype(F32) * line, axis=1, keepdims=True)

    logit = lax.fori_loop(0, ROWS, score_part, jnp.zeros((slots, 1), F32))
    score = 1.0 / (1.0 + jnp.exp(-logit))

    def expert_part(s, sums):
        gate, upper = sums
        scaled = (taken[s].astype(F32) * score).astype(BF16)
        features = pl.ds(pl.multiple_of(owner(s) * width, 128), width)
        return gate + dot(scaled, wg[features, :]), upper + dot(scaled, wu[features, :])

    zero = jnp.zeros((slots, wg.shape[1]), F32)
    gate, upper = lax.fori_loop(0, ROWS, expert_part, (zero, zero))
    hid_e[...] = (silu(gate) * upper).astype(BF16)

    def d_copy(q, s, cross):
        target = to_row(s // 2, s % 2) | ({"core": 1 - core} if cross else {})
        return remote(
            mine_h[q].at[his if cross else mine], hid[q].at[s, :, units(q, core)],
            d_send.at[q], d_recv.at[q, s, cross], target,
        )

    def d_arrival(q, s, cross):
        there = units(q, 1 - core if cross else core)
        return remote(mine_h[q].at[mine], hid[q].at[s, :, there], d_send.at[q], d_recv.at[q, s, cross], other_y)

    def d_relay(q, dx):
        s = dx * 2 + 1
        return remote(hid[q].at[1], hid[q].at[s], d_send.at[q], d_recv.at[q, s, 0], to_row(dx, 0))

    def block_end(q):
        gate, upper = pair_sum(q, 0)
        for dx in (2, 1, 3):
            x_copy(q, dx).wait_recv()
            gate = gate + xrecv[q][dx - 1, :, : sizes[q]].astype(F32)
            upper = upper + xrecv[q][dx - 1, :, sizes[q] :].astype(F32)
        mine_h[q][...] = (silu(gate) * upper).astype(BF16)
        hid[q][0, :, units(q, core)] = mine_h[q][mine, :]
        for s in (1, 2, 6, 0) if q == 0 else (1, 2, 6, 4, 0):
            for cross in (0, 1):
                if s or cross:
                    copy = d_copy(q, s, cross)
                    copy.start()

    def block_relay(q, steps):
        for cross in (0, 1):
            d_arrival(q, 1, cross).wait_recv()
        for dx in steps:
            copy = d_relay(q, dx)
            copy.start()

    def d_onward(q, dx):
        rows = pl.ds(0 if dx == 1 else half // 2, half // 2)
        return remote(
            hid[q].at[dx * 2, rows], hid[q].at[4, rows], d_send.at[q], d_recv.at[q, 4, dx // 2], {"x": ahead(dx)}
        )

    def block_across(q, dx):
        s = dx * 2
        for cross in (0, 1):
            d_arrival(q, s, cross).wait_recv()
        d_onward(q, dx).start()
        copy = remote(hid[q].at[s], hid[q].at[s + 1], d_send.at[q], d_recv.at[q, s + 1, 0], other_y)
        copy.start()

    def result_part(dx, dy):
        target = ahead(4 - dx) * 2 + lax.rem(yl + dy, 2)
        return dot(hid_e[...], wd[:, pl.ds(pl.multiple_of(target * width, 128), width)])

    def ey_copy(dx):
        return remote(eysend.at[dx], eyrecv.at[dx], ey_send, ey_recv.at[dx], other_y)

    def ex_copy(dx):
        return remote(exsend.at[dx], exrecv.at[dx], ex_send, ex_recv.at[dx], {"x": ahead(4 - dx)})

    far_copy = remote(efar, egot, ef_send, ef_recv, {"x": ahead(2)})

    loads[6].wait()
    efar[0] = result_part(2, 0).astype(BF16)
    efar[1] = result_part(2, 1).astype(BF16)
    far_copy.start()
    for dx in (1, 3):
        eysend[dx] = result_part(dx, 1).astype(BF16)
        ey_copy(dx).start()
    y_start(1, 0)
    for dx in (2, 1, 3):
        pair_send(1, dx)
    far_copy.wait_recv()
    eysend[0] = (result_part(0, 1) + egot[1].astype(F32)).astype(BF16)
    ey_copy(0).start()
    for dx in (1, 3):
        ey_copy(dx).wait_recv()
        exsend[dx] = (result_part(dx, 0) + eyrecv[dx].astype(F32)).astype(BF16)
        ex_copy(dx).start()
    block_end(0)
    total = result_part(0, 0) + egot[0].astype(F32)
    block_end(1)
    block_relay(0, (2,))
    ey_copy(0).wait_recv()
    total = total + eyrecv[0].astype(F32)
    for dx in (1, 3):
        ex_copy(dx).wait_recv()
        total = total + exrecv[dx].astype(F32)
    high = total.astype(BF16)
    hilo[:slots] = high
    hilo[slots : 2 * slots] = (total - high.astype(F32)).astype(BF16)
    k_copy = remote(hilo.at[: 2 * slots], hilo.at[2 * slots :], k_send, k_recv, sibling)
    k_copy.start()
    for q in (0, 1):
        loads[7 + q].wait()
        w_out[q].wait_recv()
        d_arrival(q, 0, 1).wait_recv()

    def f_copy(s, q):
        target = {"yh": lax.rem(yh + q // 4, 2), "z": lax.rem(z + q % 4, 4)}
        return remote(fsend.at[s], frecv.at[q - 1], f_send, f_recv.at[q - 1], target)

    def begin(s):
        tokens_of = pl.ds(pl.multiple_of(owner(s) * block + core * half, half), half)
        return dot(hid[0][s], sd[0][...]) + dot(place[tokens_of, :], hilo[...])

    def finish(s, begun=None):
        j = owner(s)
        total = (begin(s) if begun is None else begun) + dot(hid[1][s], sd[1][...])
        q = lax.rem(j // 4 + yh, 2) * 4 + lax.rem(lax.rem(j, 4) + 4 - z, 4)

        @pl.when(q == 0)
        def _():
            own[...] = total

        @pl.when(q > 0)
        def _():
            fsend[s] = total.astype(BF16)
            f_copy(s, q).start()

    for dx in (1, 3):
        block_across(0, dx)
    block_relay(1, (1, 3, 2))
    k_copy.wait_recv()
    finish(0)
    finish(1)
    def end_direct(s):
        d_arrival(1, s, 0).wait_recv()
        d_arrival(1, s, 1).wait_recv()
        finish(s)

    def begin_far(dx):
        d_relay(0, dx).wait_recv()
        early[dx - 1] = begin(dx * 2 + 1)

    end_direct(2)
    end_direct(6)
    begin_far(1)
    begin_far(3)
    d_onward(0, 1).wait_recv()
    d_onward(0, 3).wait_recv()
    end_direct(4)
    begin_far(2)
    for dx in (1, 3, 2):
        d_relay(1, dx).wait_recv()
        finish(dx * 2 + 1, early[dx - 1])

    total = own[...]
    for q in range(1, ROWS):
        f_copy(0, q).wait_recv()
        total = total + frecv[q - 1].astype(F32)
    out[...] = total.astype(BF16)

    def left(bytes_of, sem):
        pltpu.make_async_copy(bytes_of, bytes_of, sem).wait()

    left(frecv, a_send)
    left(frecv, s_send)
    left(frecv, b_send)
    for q in (0, 1):
        left(ysend[q], y_send.at[q])
        left(xsend[q], x_send.at[q])
        left(xs.at[:3, :, : 5 * sizes[q] // 2], d_send.at[q])
        w_out[q].wait_send()
    left(eysend.at[:3], ey_send)
    left(eysend.at[:2], ex_send)
    far_copy.wait_send()
    k_copy.wait_send()
    left(frecv, f_send)


def per_device(tokens, expert_ids, modality, tile_counts, router, w_gate, w_up, w_down, shared_gate, shared_up, shared_down):
    block, depth = tokens.shape
    width = shared_down.shape[1]
    hidden = shared_gate.shape[1]
    inner = w_gate.shape[2]
    slots = 2 * MAXT * TILE
    half = block // 2
    sizes = (256, hidden - 256)
    count = expert_ids.shape[0]
    vmem = pl.BlockSpec(memory_space=pltpu.VMEM)
    hbm = pl.BlockSpec(memory_space=pl.ANY)
    dma = pltpu.SemaphoreType.DMA
    return pl.pallas_call(
        kernel,
        name="layer",
        out_shape=pltpu.VMEM((half, width), BF16),
        in_specs=[vmem, vmem, pl.BlockSpec(memory_space=pltpu.SMEM), hbm, vmem] + [hbm] * 6,
        out_specs=vmem,
        scratch_shapes=[
            pltpu.VMEM((block, depth), BF16),
            pltpu.VMEM((depth, inner), BF16),
            pltpu.VMEM((depth, inner), BF16),
            pltpu.VMEM((inner, depth), BF16),
            pltpu.VMEM((width, hidden), BF16),
            pltpu.VMEM((width, hidden), BF16),
            *(pltpu.VMEM((2 * size, width), BF16) for size in sizes),
            pltpu.VMEM((ROWS, block, width), BF16),
            pltpu.VMEM((slots, count), BF16),
            pltpu.VMEM((count, 4 * slots), BF16),
            *(pltpu.VMEM((4, block, 2 * size), BF16) for size in sizes + sizes),
            *(pltpu.VMEM((3, block, 2 * size), BF16) for size in sizes + sizes),
            pltpu.VMEM((ROWS, slots, width), BF16),
            pltpu.VMEM((slots, inner), BF16),
            pltpu.VMEM((4, slots, width), BF16),
            pltpu.VMEM((4, slots, width), BF16),
            pltpu.VMEM((4, slots, width), BF16),
            pltpu.VMEM((4, slots, width), BF16),
            pltpu.VMEM((2, slots, width), BF16),
            pltpu.VMEM((2, slots, width), BF16),
            pltpu.VMEM((4 * slots, width), BF16),
            *(pltpu.VMEM((block, size), BF16) for size in sizes),
            *(pltpu.VMEM((ROWS, half, 2 * size), BF16) for size in sizes),
            pltpu.VMEM((3, half, width), F32),
            pltpu.VMEM((half, width), F32),
            pltpu.VMEM((ROWS, half, width), BF16),
            pltpu.VMEM((ROWS - 1, half, width), BF16),
            dma((10,)),
            dma, dma((ROWS,)), dma, dma((ROWS,)),
            dma((2,)), dma((2, 4)), dma((2,)), dma((2, 3)),
            dma, dma((ROWS,)),
            dma, dma((4,)), dma, dma((4,)), dma, dma,
            dma((2,)), dma((2, ROWS, 2)), dma((2,)), dma((2,)), dma, dma, dma, dma((ROWS - 1,)),
        ],
        compiler_params=pltpu.CompilerParams(
            collective_id=0, has_side_effects=True, vmem_limit_bytes=60 * 1024 * 1024
        ),
    )(
        expert_ids.reshape(1, count), modality.reshape(1, count), tile_counts, tokens, router.reshape(1, depth),
        w_gate, w_up, w_down, shared_gate, shared_up, shared_down,
    )


def solution(mesh):
    split = Mesh(mesh.devices.reshape(4, 2, 2, 4, 2), ("x", "yl", "yh", "z", "core"))
    placed = (
        P(ROW, None),
        P(),
        P(),
        P(),
        P(None, COL),
        P(COL, None, ROW),
        P(COL, None, ROW),
        P(COL, ROW, None),
        P(ROW, COL),
        P(ROW, COL),
        P(COL, ROW),
    )
    return jax.shard_map(
        per_device, mesh=split, in_specs=placed, out_specs=P(COL, ROW), check_vma=False
    )
```

```python
import jax
import jax.numpy as jnp
from jax import lax
from jax.experimental import pallas as pl
from jax.experimental.pallas import tpu as pltpu
from jax.sharding import Mesh
from jax.sharding import PartitionSpec as P

TILE = 8
MAXT = 4
ROW = ("x", "yl")
COL = ("yh", "z", "core")
ROWS = 8
MESH = pl.DeviceIdType.MESH
BF16 = jnp.bfloat16
F32 = jnp.float32


def dot(a, b):
    return jnp.dot(a, b, preferred_element_type=F32)


def silu(v):
    return v / (1.0 + jnp.exp(-v))


def kernel(
    ids, mod, counts, tokens, router, w_gate, w_up, w_down, s_gate, s_up, s_down,
    out,
    rows_in, wg, wu, wd, sg, su, sd, xs, table, place,
    ysend0, ysend1, yrecv0, yrecv1, xsend0, xsend1, xrecv0, xrecv1, taken,
    hid_e, eysend, eyrecv, exsend, exrecv, efar, egot, hilo, mine_h0, mine_h1, hid0, hid1, own, fsend, frecv,
    load_sem, a_send, a_recv, s_send, s_recv, y_send, y_recv, x_send, x_recv, b_send, b_recv,
    ey_send, ey_recv, ex_send, ex_recv, ef_send, ef_recv, d_send, d_recv, w_send, w_recv, k_send, k_recv, f_send, f_recv,
):
    x, yl, yh = lax.axis_index("x"), lax.axis_index("yl"), lax.axis_index("yh")
    z, core = lax.axis_index("z"), lax.axis_index("core")
    block, width = xs.shape[1], xs.shape[2]
    half = block // 2
    slots = table.shape[0]
    mine_h, hid = (mine_h0, mine_h1), (hid0, hid1)
    ysend, yrecv, xsend, xrecv = (ysend0, ysend1), (yrecv0, yrecv1), (xsend0, xsend1), (xrecv0, xrecv1)
    quarter, hidden = half // 2, sg.shape[1]
    row = x * 2 + yl
    expert = yh * 8 + z * 2 + core

    def ahead(dx):
        return lax.rem(x + dx, 4)

    def owner(slot):
        dx, dy = slot // 2, slot % 2
        return lax.rem(x + 4 - dx, 4) * 2 + (yl + dy) % 2

    def to_row(dx, dy):
        return {"x": ahead(dx), "yl": lax.rem(yl + dy, 2)}

    sibling = {"core": 1 - core}
    other_y = {"yl": 1 - yl}

    def remote(src, dst, send, recv, device):
        return pltpu.make_async_remote_copy(
            src_ref=src, dst_ref=dst, send_sem=send, recv_sem=recv, device_id=device, device_id_type=MESH
        )

    def units(of):
        return pl.ds(pl.multiple_of(of * hidden, hidden), hidden)

    def rows_of(of):
        return pl.ds(pl.multiple_of(of * quarter, quarter), quarter)

    loads = [
        pltpu.make_async_copy(tokens, rows_in, load_sem.at[0]),
        pltpu.make_async_copy(tokens.at[:, pl.ds(pl.multiple_of(row * width, 128), width)], xs.at[0], load_sem.at[9]),
        pltpu.make_async_copy(s_gate, sg, load_sem.at[1]),
        pltpu.make_async_copy(s_up, su, load_sem.at[2]),
        pltpu.make_async_copy(w_gate.at[0], wg, load_sem.at[3]),
        pltpu.make_async_copy(w_up.at[0], wu, load_sem.at[4]),
        pltpu.make_async_copy(w_down.at[0], wd, load_sem.at[5]),
        pltpu.make_async_copy(s_down, sd.at[units(core)], load_sem.at[6]),
    ]
    for load in loads:
        load.start()

    barrier = pltpu.get_barrier_semaphore()
    peers = [to_row(s // 2, s % 2) for s in range(1, ROWS)]
    peers += [to_row(s // 2, s % 2) | sibling for s in (1, 2, 4, 6)] + [sibling]
    peers += [{"yh": lax.rem(yh + q // 4, 2), "z": lax.rem(z + q % 4, 4)} for q in range(1, 8)]
    for peer in peers:
        pl.semaphore_signal(barrier, inc=1, device_id=peer, device_id_type=MESH)

    count = ids.shape[1]
    lane = lax.broadcasted_iota(jnp.int32, (2, count), 1)
    kind = lax.broadcasted_iota(jnp.int32, (2, count), 0)
    at = lax.broadcasted_iota(jnp.int32, (slots, count), 0)

    def ones_of(expert):
        member = (ids[...] == expert) & (mod[...] == kind)
        rank = member.astype(jnp.int32)
        step = 1
        while step < count:
            rank = rank + jnp.where(lane >= step, pltpu.roll(rank, step, 1), 0)
            step *= 2
        rank = rank - 1
        limit = jnp.where(kind == 0, counts[0, expert], counts[1, expert]) * TILE
        spot = jnp.where(member & (rank < limit), kind * (MAXT * TILE) + rank, -1)
        return (at == jnp.maximum(spot[0:1, :], spot[1:2, :])).astype(F32)

    pl.semaphore_wait(barrier, len(peers))

    mine = pl.ds(pl.multiple_of(core * half, half), half)
    his = pl.ds(pl.multiple_of((1 - core) * half, half), half)

    def a_copy(s):
        dx, dy = s // 2, s % 2
        target = ahead(dx) * 2 + lax.rem(yl + dy, 2)
        return remote(
            rows_in.at[mine, pl.ds(pl.multiple_of(target * width, 128), width)],
            xs.at[s, mine], a_send, a_recv.at[s], to_row(dx, dy),
        )

    def s_copy(s):
        return remote(xs.at[s, mine], xs.at[s, mine], s_send, s_recv.at[s], sibling)

    def s_arrival(s):
        return remote(xs.at[s, his], xs.at[s, his], s_send, s_recv.at[s], sibling)

    order = (5, 3, 7, 1, 4, 2, 6)
    loads[0].wait()
    for s in order:
        a_copy(s).start()

    def y_copy(q, dx):
        return remote(ysend[q].at[dx], yrecv[q].at[dx], y_send.at[q], y_recv.at[q, dx], other_y)

    def x_copy(q, dx):
        return remote(
            xsend[q].at[dx - 1], xrecv[q].at[dx - 1], x_send.at[q], x_recv.at[q, dx - 1], {"x": ahead(4 - dx)}
        )

    w_copy = remote(s_down, sd.at[units(core)], w_send, w_recv, sibling)
    w_copy.start()
    ones = ones_of(expert)
    table[...] = ones.astype(BF16)
    place[:, : 2 * slots] = jnp.concatenate([ones, ones], axis=0).T.astype(BF16)
    ones = ones_of(yh * 8 + z * 2 + 1 - core)
    place[:, 2 * slots :] = jnp.concatenate([ones, ones], axis=0).T.astype(BF16)

    def part(q, s):
        low = q * quarter
        rows = jnp.concatenate([xs[s, low : low + quarter], xs[s, half + low : half + low + quarter]], axis=0)
        return dot(rows, sg[...]), dot(rows, su[...])

    def y_start(q, dx):
        gate, upper = part(q, dx * 2 + 1)
        ysend[q][dx, :, :hidden] = gate.astype(BF16)
        ysend[q][dx, :, hidden:] = upper.astype(BF16)
        y_copy(q, dx).start()

    for load in loads[1:4]:
        load.wait()
    for s in order[:2]:
        a_copy(s).wait_recv()
        s_copy(s).start()
    s_arrival(order[0]).wait_recv()
    y_start(0, 2)
    for s in order[2:]:
        a_copy(s).wait_recv()
        s_copy(s).start()

    def part_of(s):
        columns = pl.ds(pl.multiple_of(owner(s) * block, 128), block)
        return dot(table[:, columns], xs[s])

    rows = part_of(0)
    for i, s in enumerate(order):
        if i > 0:
            s_arrival(s).wait_recv()
        rows = rows + part_of(s)
    taken[0] = rows.astype(BF16)

    def b_copy(source, dx, dy):
        s = dx * 2 + dy if source == 0 else dx * 2 + 1
        return remote(taken.at[source], taken.at[s], b_send, b_recv.at[s], to_row(dx, dy))

    def b_arrival(s):
        return remote(taken.at[s], taken.at[s], b_send, b_recv.at[s], other_y)

    b_out = [b_copy(0, 0, 1), b_copy(0, 2, 0), b_copy(0, 1, 0), b_copy(0, 3, 0)]
    for copy in b_out:
        copy.start()

    for q, dx in ((0, 1), (0, 3), (0, 0), (1, 2), (1, 1), (1, 3)):
        y_start(q, dx)

    def pair_sum(q, dx):
        y_copy(q, dx).wait_recv()
        gate, upper = part(q, dx * 2)
        return gate + yrecv[q][dx, :, :hidden].astype(F32), upper + yrecv[q][dx, :, hidden:].astype(F32)

    def pair_send(q, dx):
        gate, upper = pair_sum(q, dx)
        xsend[q][dx - 1, :, :hidden] = gate.astype(BF16)
        xsend[q][dx - 1, :, hidden:] = upper.astype(BF16)
        x_copy(q, dx).start()

    b_arrival(1).wait_recv()
    relayed = [b_copy(1, dx, 0) for dx in (2, 1, 3)]
    for copy in relayed:
        copy.start()
    b_out += relayed
    for dx in (2, 1, 3):
        pair_send(0, dx)

    for s in (2, 3, 4, 5, 6, 7):
        b_arrival(s).wait_recv()
    loads[4].wait()
    loads[5].wait()

    def score_part(s, total):
        line = router[:, pl.ds(pl.multiple_of(owner(s) * width, 128), width)].astype(F32)
        return total + jnp.sum(taken[s].astype(F32) * line, axis=1, keepdims=True)

    logit = lax.fori_loop(0, ROWS, score_part, jnp.zeros((slots, 1), F32))
    score = 1.0 / (1.0 + jnp.exp(-logit))

    def expert_part(s, sums):
        gate, upper = sums
        scaled = (taken[s].astype(F32) * score).astype(BF16)
        features = pl.ds(pl.multiple_of(owner(s) * width, 128), width)
        return gate + dot(scaled, wg[features, :]), upper + dot(scaled, wu[features, :])

    zero = jnp.zeros((slots, wg.shape[1]), F32)
    gate, upper = lax.fori_loop(0, ROWS, expert_part, (zero, zero))
    hid_e[...] = (silu(gate) * upper).astype(BF16)

    def d_copy(q, s, cross):
        target = to_row(s // 2, s % 2) | ({"core": 1 - core} if cross else {})
        return remote(
            mine_h[q].at[rows_of(1 - core if cross else core)], hid[q].at[s, :, units(core)],
            d_send.at[q], d_recv.at[q, s, cross], target,
        )

    def d_arrival(q, s, cross):
        there = units(1 - core if cross else core)
        return remote(mine_h[q].at[rows_of(core)], hid[q].at[s, :, there], d_send.at[q], d_recv.at[q, s, cross], other_y)

    def d_relay(q, dx):
        s = dx * 2 + 1
        return remote(hid[q].at[1], hid[q].at[s], d_send.at[q], d_recv.at[q, s, 0], to_row(dx, 0))

    def block_end(q):
        gate, upper = pair_sum(q, 0)
        for dx in (2, 1, 3):
            x_copy(q, dx).wait_recv()
            gate = gate + xrecv[q][dx - 1, :, :hidden].astype(F32)
            upper = upper + xrecv[q][dx - 1, :, hidden:].astype(F32)
        mine_h[q][...] = (silu(gate) * upper).astype(BF16)
        hid[q][0, :, units(core)] = mine_h[q][rows_of(core), :]
        for s in (1, 2, 6, 0) if q == 0 else (1, 2, 6, 4, 0):
            for cross in (0, 1):
                if s or cross:
                    copy = d_copy(q, s, cross)
                    copy.start()

    def block_relay(q, steps):
        for cross in (0, 1):
            d_arrival(q, 1, cross).wait_recv()
        for dx in steps:
            copy = d_relay(q, dx)
            copy.start()

    def d_onward(q, dx):
        rows = pl.ds(0 if dx == 1 else quarter // 2, quarter // 2)
        return remote(
            hid[q].at[dx * 2, rows], hid[q].at[4, rows], d_send.at[q], d_recv.at[q, 4, dx // 2], {"x": ahead(dx)}
        )

    def block_across(q, dx):
        s = dx * 2
        for cross in (0, 1):
            d_arrival(q, s, cross).wait_recv()
        d_onward(q, dx).start()
        copy = remote(hid[q].at[s], hid[q].at[s + 1], d_send.at[q], d_recv.at[q, s + 1, 0], other_y)
        copy.start()

    def result_part(dx, dy):
        target = ahead(4 - dx) * 2 + lax.rem(yl + dy, 2)
        return dot(hid_e[...], wd[:, pl.ds(pl.multiple_of(target * width, 128), width)])

    def ey_copy(dx):
        return remote(eysend.at[dx], eyrecv.at[dx], ey_send, ey_recv.at[dx], other_y)

    def ex_copy(dx):
        return remote(exsend.at[dx], exrecv.at[dx], ex_send, ex_recv.at[dx], {"x": ahead(4 - dx)})

    far_copy = remote(efar, egot, ef_send, ef_recv, {"x": ahead(2)})

    loads[6].wait()
    efar[0] = result_part(2, 0).astype(BF16)
    efar[1] = result_part(2, 1).astype(BF16)
    far_copy.start()
    for dx in (1, 3):
        eysend[dx] = result_part(dx, 1).astype(BF16)
        ey_copy(dx).start()
    y_start(1, 0)
    for dx in (2, 1, 3):
        pair_send(1, dx)
    far_copy.wait_recv()
    eysend[0] = (result_part(0, 1) + egot[1].astype(F32)).astype(BF16)
    ey_copy(0).start()
    for dx in (1, 3):
        ey_copy(dx).wait_recv()
        exsend[dx] = (result_part(dx, 0) + eyrecv[dx].astype(F32)).astype(BF16)
        ex_copy(dx).start()
    block_end(0)
    total = result_part(0, 0) + egot[0].astype(F32)
    block_end(1)
    block_relay(0, (2,))
    ey_copy(0).wait_recv()
    total = total + eyrecv[0].astype(F32)
    for dx in (1, 3):
        ex_copy(dx).wait_recv()
        total = total + exrecv[dx].astype(F32)
    high = total.astype(BF16)
    hilo[:slots] = high
    hilo[slots : 2 * slots] = (total - high.astype(F32)).astype(BF16)
    k_copy = remote(hilo.at[: 2 * slots], hilo.at[2 * slots :], k_send, k_recv, sibling)
    k_copy.start()
    loads[7].wait()
    w_copy.wait_recv()
    for q in (0, 1):
        d_arrival(q, 0, 1).wait_recv()

    def f_copy(q, s, to):
        target = {"yh": lax.rem(yh + to // 4, 2), "z": lax.rem(z + to % 4, 4)}
        return remote(fsend.at[q, s], frecv.at[q, to - 1], f_send.at[q], f_recv.at[q, to - 1], target)

    def finish(s, chunks):
        j = owner(s)
        count = quarter * len(chunks)
        tokens_of = pl.ds(pl.multiple_of(j * block + core * half + chunks[0] * quarter, quarter), count)
        units_of = hid[chunks[0]][s] if len(chunks) == 1 else jnp.concatenate([hid0[s], hid1[s]], axis=0)
        total = dot(units_of, sd[...]) + dot(place[tokens_of, :], hilo[...])
        to = lax.rem(j // 4 + yh, 2) * 4 + lax.rem(lax.rem(j, 4) + 4 - z, 4)

        @pl.when(to == 0)
        def _():
            for i, q in enumerate(chunks):
                own[q] = total[i * quarter : (i + 1) * quarter]

        @pl.when(to > 0)
        def _():
            for i, q in enumerate(chunks):
                fsend[q, s] = total[i * quarter : (i + 1) * quarter].astype(BF16)
                f_copy(q, s, to).start()

    for dx in (1, 3):
        block_across(0, dx)
    block_relay(1, (1, 3, 2))
    k_copy.wait_recv()
    finish(0, (0, 1))
    finish(1, (0, 1))

    def end_direct(s):
        d_arrival(1, s, 0).wait_recv()
        d_arrival(1, s, 1).wait_recv()
        finish(s, (0, 1))

    def end_far(q, dx):
        d_relay(q, dx).wait_recv()
        finish(dx * 2 + 1, (q,))

    end_direct(2)
    end_direct(6)
    end_far(0, 1)
    end_far(0, 3)
    d_onward(0, 1).wait_recv()
    d_onward(0, 3).wait_recv()
    end_direct(4)
    end_far(0, 2)
    for dx in (1, 3, 2):
        end_far(1, dx)

    for q in (0, 1):
        total = own[q]
        for to in range(1, ROWS):
            f_copy(q, 0, to).wait_recv()
            total = total + frecv[q, to - 1].astype(F32)
        out[q * quarter : (q + 1) * quarter, :] = total.astype(BF16)

    def left(bytes_of, sem):
        pltpu.make_async_copy(bytes_of, bytes_of, sem).wait()

    left(frecv, a_send)
    left(frecv, s_send)
    left(frecv, b_send)
    for q in (0, 1):
        left(ysend[q], y_send.at[q])
        left(xsend[q], x_send.at[q])
        left(xs.at[:3], d_send.at[q])
        left(frecv.at[q], f_send.at[q])
    left(eysend.at[:3], ey_send)
    left(eysend.at[:2], ex_send)
    far_copy.wait_send()
    k_copy.wait_send()
    w_copy.wait_send()


def per_device(tokens, expert_ids, modality, tile_counts, router, w_gate, w_up, w_down, shared_gate, shared_up, shared_down):
    block, depth = tokens.shape
    width = shared_down.shape[1]
    hidden = shared_gate.shape[1]
    inner = w_gate.shape[2]
    slots = 2 * MAXT * TILE
    half = block // 2
    quarter = half // 2
    count = expert_ids.shape[0]
    vmem = pl.BlockSpec(memory_space=pltpu.VMEM)
    hbm = pl.BlockSpec(memory_space=pl.ANY)
    dma = pltpu.SemaphoreType.DMA
    return pl.pallas_call(
        kernel,
        name="layer",
        out_shape=pltpu.VMEM((half, width), BF16),
        in_specs=[vmem, vmem, pl.BlockSpec(memory_space=pltpu.SMEM), hbm, vmem] + [hbm] * 6,
        out_specs=vmem,
        scratch_shapes=[
            pltpu.VMEM((block, depth), BF16),
            pltpu.VMEM((depth, inner), BF16),
            pltpu.VMEM((depth, inner), BF16),
            pltpu.VMEM((inner, depth), BF16),
            pltpu.VMEM((width, hidden), BF16),
            pltpu.VMEM((width, hidden), BF16),
            pltpu.VMEM((2 * hidden, width), BF16),
            pltpu.VMEM((ROWS, block, width), BF16),
            pltpu.VMEM((slots, count), BF16),
            pltpu.VMEM((count, 4 * slots), BF16),
            *[pltpu.VMEM((4, half, 2 * hidden), BF16)] * 4,
            *[pltpu.VMEM((3, half, 2 * hidden), BF16)] * 4,
            pltpu.VMEM((ROWS, slots, width), BF16),
            pltpu.VMEM((slots, inner), BF16),
            pltpu.VMEM((4, slots, width), BF16),
            pltpu.VMEM((4, slots, width), BF16),
            pltpu.VMEM((4, slots, width), BF16),
            pltpu.VMEM((4, slots, width), BF16),
            pltpu.VMEM((2, slots, width), BF16),
            pltpu.VMEM((2, slots, width), BF16),
            pltpu.VMEM((4 * slots, width), BF16),
            *[pltpu.VMEM((half, hidden), BF16)] * 2,
            *[pltpu.VMEM((ROWS, quarter, 2 * hidden), BF16)] * 2,
            pltpu.VMEM((2, quarter, width), F32),
            pltpu.VMEM((2, ROWS, quarter, width), BF16),
            pltpu.VMEM((2, ROWS - 1, quarter, width), BF16),
            dma((10,)),
            dma, dma((ROWS,)), dma, dma((ROWS,)),
            dma((2,)), dma((2, 4)), dma((2,)), dma((2, 3)),
            dma, dma((ROWS,)),
            dma, dma((4,)), dma, dma((4,)), dma, dma,
            dma((2,)), dma((2, ROWS, 2)), dma, dma, dma, dma, dma((2,)), dma((2, ROWS - 1)),
        ],
        compiler_params=pltpu.CompilerParams(
            collective_id=0, has_side_effects=True, vmem_limit_bytes=60 * 1024 * 1024
        ),
    )(
        expert_ids.reshape(1, count), modality.reshape(1, count), tile_counts, tokens, router.reshape(1, depth),
        w_gate, w_up, w_down, shared_gate, shared_up, shared_down,
    )


def solution(mesh):
    split = Mesh(mesh.devices.reshape(4, 2, 2, 4, 2), ("x", "yl", "yh", "z", "core"))
    placed = (
        P(ROW, None),
        P(),
        P(),
        P(),
        P(None, COL),
        P(COL, None, ROW),
        P(COL, None, ROW),
        P(COL, ROW, None),
        P(ROW, COL),
        P(ROW, COL),
        P(COL, ROW),
    )
    return jax.shard_map(
        per_device, mesh=split, in_specs=placed, out_specs=P(COL, ROW), check_vma=False
    )
```

```python
import jax
import jax.numpy as jnp
from jax import lax
from jax.experimental import pallas as pl
from jax.experimental.pallas import tpu as pltpu
from jax.sharding import Mesh
from jax.sharding import PartitionSpec as P

TILE = 8
MAXT = 4
ROW = ("x", "yl")
COL = ("yh", "z", "core")
ROWS = 8
MESH = pl.DeviceIdType.MESH
BF16 = jnp.bfloat16
F32 = jnp.float32


def dot(a, b):
    return jnp.dot(a, b, preferred_element_type=F32)


def silu(v):
    return v / (1.0 + jnp.exp(-v))


def kernel(
    ids, mod, counts, tokens, router, w_gate, w_up, w_down, s_gate, s_up, s_down,
    out,
    rows_in, wg, wu, wd, sg, su, sd, xs, table, place,
    ysend0, ysend1, yrecv0, yrecv1, xsend0, xsend1, xrecv0, xrecv1, taken,
    hid_e, eysend, eyrecv, exsend, exrecv, efar, egot, hilo, mine_h0, mine_h1, hid0, hid1, own, fsend, frecv,
    load_sem, a_send, a_recv, s_send, s_recv, y_send, y_recv, x_send, x_recv, b_send, b_recv,
    ey_send, ey_recv, ex_send, ex_recv, ef_send, ef_recv, d_send, d_recv, w_send, w_recv, k_send, k_recv, f_send, f_recv,
):
    x, yl, yh = lax.axis_index("x"), lax.axis_index("yl"), lax.axis_index("yh")
    z, core = lax.axis_index("z"), lax.axis_index("core")
    block, width = xs.shape[1], xs.shape[2]
    half = block // 2
    slots = table.shape[0]
    mine_h, hid = (mine_h0, mine_h1), (hid0, hid1)
    ysend, yrecv, xsend, xrecv = (ysend0, ysend1), (yrecv0, yrecv1), (xsend0, xsend1), (xrecv0, xrecv1)
    quarter, hidden = half // 2, sg.shape[1]
    row = x * 2 + yl
    expert = yh * 8 + z * 2 + core

    def ahead(dx):
        return lax.rem(x + dx, 4)

    def owner(slot):
        dx, dy = slot // 2, slot % 2
        return lax.rem(x + 4 - dx, 4) * 2 + (yl + dy) % 2

    def to_row(dx, dy):
        return {"x": ahead(dx), "yl": lax.rem(yl + dy, 2)}

    sibling = {"core": 1 - core}
    other_y = {"yl": 1 - yl}

    def remote(src, dst, send, recv, device):
        return pltpu.make_async_remote_copy(
            src_ref=src, dst_ref=dst, send_sem=send, recv_sem=recv, device_id=device, device_id_type=MESH
        )

    def units(of):
        return pl.ds(pl.multiple_of(of * hidden, hidden), hidden)

    def rows_of(of):
        return pl.ds(pl.multiple_of(of * quarter, quarter), quarter)

    loads = [
        pltpu.make_async_copy(tokens, rows_in, load_sem.at[0]),
        pltpu.make_async_copy(tokens.at[:, pl.ds(pl.multiple_of(row * width, 128), width)], xs.at[0], load_sem.at[9]),
        pltpu.make_async_copy(s_gate, sg, load_sem.at[1]),
        pltpu.make_async_copy(s_up, su, load_sem.at[2]),
        pltpu.make_async_copy(w_gate.at[0], wg, load_sem.at[3]),
        pltpu.make_async_copy(w_up.at[0], wu, load_sem.at[4]),
        pltpu.make_async_copy(w_down.at[0], wd, load_sem.at[5]),
        pltpu.make_async_copy(s_down, sd.at[units(core)], load_sem.at[6]),
    ]
    for load in loads:
        load.start()

    barrier = pltpu.get_barrier_semaphore()
    peers = [to_row(s // 2, s % 2) for s in range(1, ROWS)]
    peers += [to_row(s // 2, s % 2) | sibling for s in (1, 2, 4, 6)] + [sibling]
    peers += [{"yh": lax.rem(yh + q // 4, 2), "z": lax.rem(z + q % 4, 4)} for q in range(1, 8)]
    for peer in peers:
        pl.semaphore_signal(barrier, inc=1, device_id=peer, device_id_type=MESH)

    count = ids.shape[1]
    lane = lax.broadcasted_iota(jnp.int32, (2, count), 1)
    kind = lax.broadcasted_iota(jnp.int32, (2, count), 0)
    at = lax.broadcasted_iota(jnp.int32, (slots, count), 0)

    def ones_of(expert):
        member = (ids[...] == expert) & (mod[...] == kind)
        rank = member.astype(jnp.int32)
        step = 1
        while step < count:
            rank = rank + jnp.where(lane >= step, pltpu.roll(rank, step, 1), 0)
            step *= 2
        rank = rank - 1
        limit = jnp.where(kind == 0, counts[0, expert], counts[1, expert]) * TILE
        spot = jnp.where(member & (rank < limit), kind * (MAXT * TILE) + rank, -1)
        return (at == jnp.maximum(spot[0:1, :], spot[1:2, :])).astype(F32)

    pl.semaphore_wait(barrier, len(peers))

    mine = pl.ds(pl.multiple_of(core * half, half), half)
    his = pl.ds(pl.multiple_of((1 - core) * half, half), half)

    def a_copy(s):
        dx, dy = s // 2, s % 2
        target = ahead(dx) * 2 + lax.rem(yl + dy, 2)
        return remote(
            rows_in.at[mine, pl.ds(pl.multiple_of(target * width, 128), width)],
            xs.at[s, mine], a_send, a_recv.at[s - 1], to_row(dx, dy),
        )

    def s_copy(s):
        return remote(xs.at[s, mine], xs.at[s, mine], s_send, s_recv.at[s - 1], sibling)

    def s_arrival(s):
        return remote(xs.at[s, his], xs.at[s, his], s_send, s_recv.at[s - 1], sibling)

    order = (5, 3, 7, 1, 4, 2, 6)
    loads[0].wait()
    for s in order:
        a_copy(s).start()

    def y_copy(q, dx):
        return remote(ysend[q].at[dx], yrecv[q].at[dx], y_send.at[q], y_recv.at[q, dx], other_y)

    def x_copy(q, dx):
        return remote(
            xsend[q].at[dx - 1], xrecv[q].at[dx - 1], x_send.at[q], x_recv.at[q, dx - 1], {"x": ahead(4 - dx)}
        )

    w_copy = remote(s_down, sd.at[units(core)], w_send, w_recv, sibling)
    w_copy.start()
    ones = ones_of(expert)
    table[...] = ones.astype(BF16)
    place[:, : 2 * slots] = jnp.concatenate([ones, ones], axis=0).T.astype(BF16)
    ones = ones_of(yh * 8 + z * 2 + 1 - core)
    place[:, 2 * slots :] = jnp.concatenate([ones, ones], axis=0).T.astype(BF16)

    def part(q, s):
        low = q * quarter
        rows = jnp.concatenate([xs[s, low : low + quarter], xs[s, half + low : half + low + quarter]], axis=0)
        return dot(rows, sg[...]), dot(rows, su[...])

    def y_start(q, dx):
        gate, upper = part(q, dx * 2 + 1)
        ysend[q][dx, :, :hidden] = gate.astype(BF16)
        ysend[q][dx, :, hidden:] = upper.astype(BF16)
        y_copy(q, dx).start()

    for load in loads[1:4]:
        load.wait()
    for s in order[:2]:
        a_copy(s).wait_recv()
        s_copy(s).start()
    s_arrival(order[0]).wait_recv()
    y_start(0, 2)
    for s in order[2:]:
        a_copy(s).wait_recv()
        s_copy(s).start()

    def part_of(s):
        columns = pl.ds(pl.multiple_of(owner(s) * block, 128), block)
        return dot(table[:, columns], xs[s])

    rows = part_of(0)
    for i, s in enumerate(order):
        if i > 0:
            s_arrival(s).wait_recv()
        rows = rows + part_of(s)
    taken[0] = rows.astype(BF16)

    def b_copy(source, dx, dy):
        s = dx * 2 + dy if source == 0 else dx * 2 + 1
        return remote(taken.at[source], taken.at[s], b_send, b_recv.at[0 if s == 1 else 1], to_row(dx, dy))

    b_out = [b_copy(0, 0, 1), b_copy(0, 2, 0), b_copy(0, 1, 0), b_copy(0, 3, 0)]
    for copy in b_out:
        copy.start()

    for q, dx in ((0, 1), (0, 3), (0, 0), (1, 2), (1, 1), (1, 3)):
        y_start(q, dx)

    def pair_sum(q, dx):
        y_copy(q, dx).wait_recv()
        gate, upper = part(q, dx * 2)
        return gate + yrecv[q][dx, :, :hidden].astype(F32), upper + yrecv[q][dx, :, hidden:].astype(F32)

    def pair_send(q, dx):
        gate, upper = pair_sum(q, dx)
        xsend[q][dx - 1, :, :hidden] = gate.astype(BF16)
        xsend[q][dx - 1, :, hidden:] = upper.astype(BF16)
        x_copy(q, dx).start()

    b_out[0].wait_recv()
    relayed = [b_copy(1, dx, 0) for dx in (2, 1, 3)]
    for copy in relayed:
        copy.start()
    b_out += relayed
    for dx in (2, 1, 3):
        pair_send(0, dx)

    pltpu.make_async_copy(taken.at[2:], taken.at[2:], b_recv.at[1]).wait()
    loads[4].wait()
    loads[5].wait()

    def score_part(s, total):
        line = router[:, pl.ds(pl.multiple_of(owner(s) * width, 128), width)].astype(F32)
        return total + jnp.sum(taken[s].astype(F32) * line, axis=1, keepdims=True)

    logit = lax.fori_loop(0, ROWS, score_part, jnp.zeros((slots, 1), F32))
    score = 1.0 / (1.0 + jnp.exp(-logit))

    def expert_part(s, sums):
        gate, upper = sums
        scaled = (taken[s].astype(F32) * score).astype(BF16)
        features = pl.ds(pl.multiple_of(owner(s) * width, 128), width)
        return gate + dot(scaled, wg[features, :]), upper + dot(scaled, wu[features, :])

    zero = jnp.zeros((slots, wg.shape[1]), F32)
    gate, upper = lax.fori_loop(0, ROWS, expert_part, (zero, zero))
    hid_e[...] = (silu(gate) * upper).astype(BF16)

    ARRIVALS = ((0, 1), (1, 0), (1, 1), (2, 0), (2, 1), (3, 0), (4, 0), (4, 1), (5, 0), (6, 0), (6, 1), (7, 0))

    def d_sem(q, s, cross):
        return d_recv.at[q, ARRIVALS.index((s, cross))]

    def d_copy(q, s, cross):
        target = to_row(s // 2, s % 2) | ({"core": 1 - core} if cross else {})
        return remote(
            mine_h[q].at[rows_of(1 - core if cross else core)], hid[q].at[s, :, units(core)],
            d_send.at[q], d_sem(q, s, cross), target,
        )

    def d_arrival(q, s, cross):
        there = units(1 - core if cross else core)
        return remote(mine_h[q].at[rows_of(core)], hid[q].at[s, :, there], d_send.at[q], d_sem(q, s, cross), other_y)

    def d_relay(q, dx):
        s = dx * 2 + 1
        return remote(hid[q].at[1], hid[q].at[s], d_send.at[q], d_sem(q, s, 0), to_row(dx, 0))

    def block_end(q):
        gate, upper = pair_sum(q, 0)
        for dx in (2, 1, 3):
            x_copy(q, dx).wait_recv()
            gate = gate + xrecv[q][dx - 1, :, :hidden].astype(F32)
            upper = upper + xrecv[q][dx - 1, :, hidden:].astype(F32)
        mine_h[q][...] = (silu(gate) * upper).astype(BF16)
        hid[q][0, :, units(core)] = mine_h[q][rows_of(core), :]
        for s in (1, 2, 6, 0) if q == 0 else (1, 2, 6, 4, 0):
            for cross in (0, 1):
                if s or cross:
                    copy = d_copy(q, s, cross)
                    copy.start()

    def block_relay(q, steps):
        for cross in (0, 1):
            d_arrival(q, 1, cross).wait_recv()
        for dx in steps:
            copy = d_relay(q, dx)
            copy.start()

    def d_onward(q, dx):
        rows = pl.ds(0 if dx == 1 else quarter // 2, quarter // 2)
        return remote(
            hid[q].at[dx * 2, rows], hid[q].at[4, rows], d_send.at[q], d_sem(q, 4, dx // 2), {"x": ahead(dx)}
        )

    def block_across(q, dx):
        s = dx * 2
        for cross in (0, 1):
            d_arrival(q, s, cross).wait_recv()
        d_onward(q, dx).start()
        copy = remote(hid[q].at[s], hid[q].at[s + 1], d_send.at[q], d_sem(q, s + 1, 0), other_y)
        copy.start()

    def result_part(dx, dy):
        target = ahead(4 - dx) * 2 + lax.rem(yl + dy, 2)
        return dot(hid_e[...], wd[:, pl.ds(pl.multiple_of(target * width, 128), width)])

    def ey_copy(dx):
        return remote(eysend.at[dx], eyrecv.at[dx], ey_send, ey_recv.at[(dx + 1) // 2], other_y)

    def ex_copy(dx):
        return remote(exsend.at[dx], exrecv.at[dx], ex_send, ex_recv.at[dx // 2], {"x": ahead(4 - dx)})

    far_copy = remote(efar, egot, ef_send, ef_recv, {"x": ahead(2)})

    loads[6].wait()
    efar[0] = result_part(2, 0).astype(BF16)
    efar[1] = result_part(2, 1).astype(BF16)
    far_copy.start()
    for dx in (1, 3):
        eysend[dx] = result_part(dx, 1).astype(BF16)
        ey_copy(dx).start()
    y_start(1, 0)
    for dx in (2, 1, 3):
        pair_send(1, dx)
    far_copy.wait_recv()
    eysend[0] = (result_part(0, 1) + egot[1].astype(F32)).astype(BF16)
    ey_copy(0).start()
    for dx in (1, 3):
        ey_copy(dx).wait_recv()
        exsend[dx] = (result_part(dx, 0) + eyrecv[dx].astype(F32)).astype(BF16)
        ex_copy(dx).start()
    block_end(0)
    total = result_part(0, 0) + egot[0].astype(F32)
    block_end(1)
    block_relay(0, (2,))
    ey_copy(0).wait_recv()
    total = total + eyrecv[0].astype(F32)
    for dx in (1, 3):
        ex_copy(dx).wait_recv()
        total = total + exrecv[dx].astype(F32)
    high = total.astype(BF16)
    hilo[:slots] = high
    hilo[slots : 2 * slots] = (total - high.astype(F32)).astype(BF16)
    k_copy = remote(hilo.at[: 2 * slots], hilo.at[2 * slots :], k_send, k_recv, sibling)
    k_copy.start()
    loads[7].wait()
    w_copy.wait_recv()
    for q in (0, 1):
        d_arrival(q, 0, 1).wait_recv()

    def f_copy(q, s, to):
        target = {"yh": lax.rem(yh + to // 4, 2), "z": lax.rem(z + to % 4, 4)}
        return remote(fsend.at[q, s], frecv.at[q, to - 1], f_send.at[q], f_recv.at[q, to - 1], target)

    def finish(s, chunks):
        j = owner(s)
        count = quarter * len(chunks)
        tokens_of = pl.ds(pl.multiple_of(j * block + core * half + chunks[0] * quarter, quarter), count)
        units_of = hid[chunks[0]][s] if len(chunks) == 1 else jnp.concatenate([hid0[s], hid1[s]], axis=0)
        total = dot(units_of, sd[...]) + dot(place[tokens_of, :], hilo[...])
        to = lax.rem(j // 4 + yh, 2) * 4 + lax.rem(lax.rem(j, 4) + 4 - z, 4)

        @pl.when(to == 0)
        def _():
            for i, q in enumerate(chunks):
                own[q] = total[i * quarter : (i + 1) * quarter]

        @pl.when(to > 0)
        def _():
            for i, q in enumerate(chunks):
                fsend[q, s] = total[i * quarter : (i + 1) * quarter].astype(BF16)
                f_copy(q, s, to).start()

    for dx in (1, 3):
        block_across(0, dx)
    block_relay(1, (1, 3, 2))
    k_copy.wait_recv()
    finish(0, (0, 1))
    finish(1, (0, 1))

    def end_direct(s):
        d_arrival(1, s, 0).wait_recv()
        d_arrival(1, s, 1).wait_recv()
        finish(s, (0, 1))

    def end_far(q, dx):
        d_relay(q, dx).wait_recv()
        finish(dx * 2 + 1, (q,))

    end_direct(2)
    end_direct(6)
    end_far(0, 1)
    end_far(0, 3)
    d_onward(0, 1).wait_recv()
    d_onward(0, 3).wait_recv()
    end_direct(4)
    end_far(0, 2)
    for dx in (1, 3, 2):
        end_far(1, dx)

    for q in (0, 1):
        total = own[q]
        for to in range(1, ROWS):
            f_copy(q, 0, to).wait_recv()
            total = total + frecv[q, to - 1].astype(F32)
        out[q * quarter : (q + 1) * quarter, :] = total.astype(BF16)

    def left(bytes_of, sem):
        pltpu.make_async_copy(bytes_of, bytes_of, sem).wait()

    left(frecv, a_send)
    left(frecv, s_send)
    left(frecv, b_send)
    for q in (0, 1):
        left(ysend[q], y_send.at[q])
        left(xsend[q], x_send.at[q])
        left(xs.at[:3], d_send.at[q])
        left(frecv.at[q], f_send.at[q])
    left(eysend.at[:3], ey_send)
    left(eysend.at[:2], ex_send)
    far_copy.wait_send()
    k_copy.wait_send()
    w_copy.wait_send()


def per_device(tokens, expert_ids, modality, tile_counts, router, w_gate, w_up, w_down, shared_gate, shared_up, shared_down):
    block, depth = tokens.shape
    width = shared_down.shape[1]
    hidden = shared_gate.shape[1]
    inner = w_gate.shape[2]
    slots = 2 * MAXT * TILE
    half = block // 2
    quarter = half // 2
    count = expert_ids.shape[0]
    vmem = pl.BlockSpec(memory_space=pltpu.VMEM)
    hbm = pl.BlockSpec(memory_space=pl.ANY)
    dma = pltpu.SemaphoreType.DMA
    return pl.pallas_call(
        kernel,
        name="layer",
        out_shape=pltpu.VMEM((half, width), BF16),
        in_specs=[vmem, vmem, pl.BlockSpec(memory_space=pltpu.SMEM), hbm, vmem] + [hbm] * 6,
        out_specs=vmem,
        scratch_shapes=[
            pltpu.VMEM((block, depth), BF16),
            pltpu.VMEM((depth, inner), BF16),
            pltpu.VMEM((depth, inner), BF16),
            pltpu.VMEM((inner, depth), BF16),
            pltpu.VMEM((width, hidden), BF16),
            pltpu.VMEM((width, hidden), BF16),
            pltpu.VMEM((2 * hidden, width), BF16),
            pltpu.VMEM((ROWS, block, width), BF16),
            pltpu.VMEM((slots, count), BF16),
            pltpu.VMEM((count, 4 * slots), BF16),
            *[pltpu.VMEM((4, half, 2 * hidden), BF16)] * 4,
            *[pltpu.VMEM((3, half, 2 * hidden), BF16)] * 4,
            pltpu.VMEM((ROWS, slots, width), BF16),
            pltpu.VMEM((slots, inner), BF16),
            pltpu.VMEM((4, slots, width), BF16),
            pltpu.VMEM((4, slots, width), BF16),
            pltpu.VMEM((4, slots, width), BF16),
            pltpu.VMEM((4, slots, width), BF16),
            pltpu.VMEM((2, slots, width), BF16),
            pltpu.VMEM((2, slots, width), BF16),
            pltpu.VMEM((4 * slots, width), BF16),
            *[pltpu.VMEM((half, hidden), BF16)] * 2,
            *[pltpu.VMEM((ROWS, quarter, 2 * hidden), BF16)] * 2,
            pltpu.VMEM((2, quarter, width), F32),
            pltpu.VMEM((2, ROWS, quarter, width), BF16),
            pltpu.VMEM((2, ROWS - 1, quarter, width), BF16),
            dma((10,)),
            dma, dma((ROWS - 1,)), dma, dma((ROWS - 1,)),
            dma((2,)), dma((2, 4)), dma((2,)), dma((2, 3)),
            dma, dma((2,)),
            dma, dma((3,)), dma, dma((2,)), dma, dma,
            dma((2,)), dma((2, 12)), dma, dma, dma, dma, dma((2,)), dma((2, ROWS - 1)),
        ],
        compiler_params=pltpu.CompilerParams(
            collective_id=0, has_side_effects=True, vmem_limit_bytes=60 * 1024 * 1024
        ),
    )(
        expert_ids.reshape(1, count), modality.reshape(1, count), tile_counts, tokens, router.reshape(1, depth),
        w_gate, w_up, w_down, shared_gate, shared_up, shared_down,
    )


def solution(mesh):
    split = Mesh(mesh.devices.reshape(4, 2, 2, 4, 2), ("x", "yl", "yh", "z", "core"))
    placed = (
        P(ROW, None),
        P(),
        P(),
        P(),
        P(None, COL),
        P(COL, None, ROW),
        P(COL, None, ROW),
        P(COL, ROW, None),
        P(ROW, COL),
        P(ROW, COL),
        P(COL, ROW),
    )
    return jax.shard_map(
        per_device, mesh=split, in_specs=placed, out_specs=P(COL, ROW), check_vma=False
    )
```
